32 devices in a mesh: nx: 4 (over x, core), ny: 4 (over z), img: 2 (over y).
Axes of the slice: x: 2, y: 2, z: 4, core: 2. Of those that a mesh axis runs over, the one named last changes fastest.
Arguments:
- features: bfloat16 [256, 8192], P(('nx', 'ny', 'img')), may hold values from 0 to 2
- link_weight: bfloat16 [3, 16, 16, 128, 128], P(None, ('nx', 'ny')), may hold values from -0.5 to 0.5
- link_row: int32 [3, 16, 16], P(None, ('nx', 'ny')), may hold values from 0 to 3
- link_col: int32 [3, 16, 16], P(None, None, ('nx', 'ny')), may hold values from 0 to 3
- link_live: int32 [3, 16, 16], P(None, ('nx', 'ny')), may hold values from 0 to 1, as said below
- bias: float32 [3, 8192], P(None, ('nx', 'ny')), may hold values from -3 to 3
Outputs:
- activations: bfloat16 [256, 8192], P(('nx', 'ny', 'img'))
The draws below stay inside these ranges and needn't reach their ends.
Inputs may be any that keep to these rules, and one draw needn't show every extreme that they name: `link_live`: in every layer at most 12 of the links of one source device are live, and exactly 12 for some source device.
All inputs are finite; a program needn't handle non-finite values.
Results may differ from the reference program's by a relative error of at most 0.0072.
Values may be sent and summed in bfloat16 or wider, within the bound.
A program may use at most 64 MiB of HBM per device.

```python
import jax
import jax.numpy as jnp
from jax import lax

BLK = 128
NB_DEV = 4
LAYERS = 3
LINKS = 16
IMAGES = 256
NEURONS = 8192
LIVE_MAX = 12


def draw_link_live(key, part):
    key_count = jax.random.fold_in(key, 11)
    key_busy = jax.random.fold_in(key, 12)
    key_perm = jax.random.fold_in(key, 13)
    live_counts = jax.random.randint(key_count, (LAYERS, LINKS), LINKS // 4, LIVE_MAX + 1)
    busiest = jax.random.randint(key_busy, (LAYERS,), 0, LINKS)
    positions = jnp.arange(LINKS, dtype=jnp.int32)
    live_counts = jnp.where(positions[None, :] == busiest[:, None], LIVE_MAX, live_counts)
    perm_keys = jax.random.split(key_perm, LAYERS * LINKS)
    ranking = jax.vmap(lambda subkey: jax.random.permutation(subkey, LINKS))(perm_keys)
    ranking = ranking.reshape(LAYERS, LINKS, LINKS)
    return (ranking < live_counts[:, :, None]).astype(jnp.int32)


def touch_ends(array, key, least, top_value):
    longest = array.shape.index(max(array.shape))
    spots = []
    for shift in (0, 1):
        where = [jax.random.randint(jax.random.fold_in(key, axis), (), 0, length) for axis, length in enumerate(array.shape)]
        where[longest] = (where[longest] + shift) % array.shape[longest]
        spots.append(tuple(where))
    return array.at[spots[0]].set(least).at[spots[1]].set(top_value)


def block_levels(key, shape, pieces, least, high):
    def one(axis_at, shards_of):
        heights = jax.random.uniform(jax.random.fold_in(jax.random.fold_in(key, 6), axis_at), (shards_of,), jnp.float32, least / len(pieces), high / len(pieces))
        return jnp.repeat(jnp.exp(heights), shape[axis_at] // shards_of).reshape((-1,) + (1,) * (len(shape) - axis_at - 1))

    level = one(*pieces[0])
    for cut in pieces[1:]:
        level = level * one(*cut)
    return level


def noise(key, extent, scale, bound, cuts=(), kind=jnp.bfloat16):
    result = jax.random.normal(key, extent, jnp.float32) * scale
    if len(cuts) > 0:
        result = block_levels(key, extent, cuts, -0.22, 0.18) * result
    return jnp.clip(result, min=-bound, max=bound).astype(kind)


def setup_inputs(seed: int = 0) -> dict:
    streams_of = jax.random.split(jax.random.key(seed), 7)
    features = jnp.clip(2.0 * jax.random.uniform(streams_of[0], (IMAGES, NEURONS), jnp.float32) ** block_levels(streams_of[0], (IMAGES, NEURONS), ((0, 32),), -0.2, 0.2), 0.0, 2.0).astype(jnp.bfloat16)
    link_weight = noise(streams_of[1], (LAYERS, LINKS, LINKS, BLK, BLK), (LINKS * BLK // 16) ** -0.5, 0.5, ((1, 16),))
    link_row = touch_ends(jax.random.randint(streams_of[2], (LAYERS, LINKS, LINKS), 0, NB_DEV), jax.random.fold_in(streams_of[2], 1), 0, NB_DEV - 1).astype(jnp.int32)
    link_col = touch_ends(jax.random.randint(streams_of[3], (LAYERS, LINKS, LINKS), 0, NB_DEV), jax.random.fold_in(streams_of[3], 1), 0, NB_DEV - 1).astype(jnp.int32)
    link_live = draw_link_live(jax.random.fold_in(streams_of[6], 71), 0)
    bias = noise(streams_of[5], (LAYERS, NEURONS), 0.5, 3.0, ((1, 16),), jnp.float32)
    return dict(features=features, link_weight=link_weight, link_row=link_row, link_col=link_col, link_live=link_live, bias=bias)


def reference(features, link_weight, link_row, link_col, link_live, bias):
    images = features.shape[0]
    nblocks = NB_DEV * LINKS
    hidden = features.reshape(images, LINKS, NB_DEV, BLK)
    for layer_idx in range(LAYERS):
        def one_source(running, inputs_now):
            source, weights, row_ids, live_mask, col_ids = inputs_now
            blocks = lax.dynamic_index_in_dim(hidden, source, 1, keepdims=False)
            masked = weights * live_mask.astype(jnp.bfloat16)[:, None, None]
            gathered = jnp.take(blocks, row_ids, axis=1)
            link_terms = jnp.einsum("ier,ers->ies", gathered.astype(jnp.float32), masked.astype(jnp.float32)).astype(jnp.bfloat16)
            targets = (jnp.arange(LINKS, dtype=jnp.int32) * NB_DEV + col_ids).astype(jnp.int32)
            running = running.at[:, targets].add(link_terms.astype(jnp.float32))
            return running, None

        sources = jnp.arange(LINKS, dtype=jnp.int32)
        start = jnp.zeros((images, nblocks, BLK), jnp.float32)
        running, unused = lax.scan(one_source, start, (sources, link_weight[layer_idx], link_row[layer_idx], link_live[layer_idx], link_col[layer_idx]))
        pre_sum = running.reshape(images, nblocks * BLK) + bias[layer_idx][None, :]
        hidden = jnp.maximum(pre_sum, 0.0).astype(jnp.bfloat16).reshape(images, LINKS, NB_DEV, BLK)
    return hidden.reshape(images, nblocks * BLK)
```

```python
import functools

import jax
import jax.numpy as jnp
from jax import lax
from jax.experimental import pallas as pl
from jax.experimental.pallas import tpu as pltpu
from jax.sharding import PartitionSpec as P

MESH = pl.DeviceIdType.MESH
CHUNKS = 2


def combine_links(received, col_ids, width):
    onehot = (col_ids[:, None] == jnp.arange(width, dtype=jnp.int32)[None, :]).astype(jnp.bfloat16)
    summed = jnp.einsum("dq,dis->iqs", onehot, received, preferred_element_type=jnp.float32)
    return summed.reshape(summed.shape[0], width * received.shape[2])


def link_products(blocks, weights, row_ids, live_mask):
    masked = weights * live_mask.astype(jnp.bfloat16)[:, None, None]
    gathered = jnp.take(blocks, row_ids, axis=1)
    result = jnp.einsum(
        "ier,ers->eis", gathered, masked, preferred_element_type=jnp.float32
    ).astype(jnp.bfloat16)
    return result


def local(features, link_weight, link_row, link_col, link_live, bias):
    block_size = link_weight.shape[-1]
    width = bias.shape[1] // block_size
    hidden = lax.all_to_all(features, ("nx", "ny"), split_axis=1, concat_axis=0, tiled=True)
    image_rows = hidden.shape[0]
    for layer_idx in range(bias.shape[0]):
        blocks = hidden.reshape(image_rows, width, block_size)
        link_terms = link_products(
            blocks, link_weight[layer_idx, 0], link_row[layer_idx, 0], link_live[layer_idx, 0]
        )
        col_ids = link_col[layer_idx, :, 0]
        summed = combine_links(
            lax.all_to_all(link_terms, ("nx", "ny"), split_axis=0, concat_axis=0, tiled=True),
            col_ids,
            width,
        )
        hidden = jnp.maximum(summed + bias[layer_idx][None, :], 0.0).astype(jnp.bfloat16)
    finished = lax.all_to_all(hidden, ("nx", "ny"), split_axis=0, concat_axis=1, tiled=True)
    return finished


def kernel(nx, ny, feat_hbm, weight_hbm, row_hbm, col_hbm, live_hbm, bias_hbm, out, feat, row, col, live, bias, isem, w, fsend, fin, act, tsend, trecv, osend, orecv,
           aux, auxs, colx, rsend, rrecv, psend, precv, colr, wsem, fs, fr, xs, xr, ts, tr, os, orr, rs, rr, ps, pr):
    nd = nx * ny
    layers = bias.shape[0]
    block = w.shape[-1]
    width = bias.shape[1] // block
    rows = feat.shape[0]
    images = rows * nd
    half = images // CHUNKS
    per = nd // CHUNKS
    f32 = jnp.float32
    my_x, my_z = lax.axis_index("nx"), lax.axis_index("ny")
    me = my_x * ny + my_z

    hz = ny // 2
    hi, lo = my_z // hz, my_z % hz
    zs = [(1 - hi) * hz + (lo + i) % hz for i in range(hz)] + [hi * hz + (lo + i) % hz for i in range(1, hz)] + [my_z]
    peers = [((my_x + i) % nx, z, i == 0 and n == ny - 1) for n, z in enumerate(zs) for i in list(range(1, nx)) + [0]]

    def place(a, b):
        return (a % CHUNKS) * per + (a // CHUNKS) * ny + b

    def at(a, b):
        return {"nx": a, "ny": b}

    my_place = place(my_x, my_z)

    loads = [
        pltpu.make_async_copy(src, dst, isem.at[n])
        for n, (src, dst) in enumerate(((feat_hbm, feat), (bias_hbm, bias), (col_hbm, col), (row_hbm, row), (live_hbm, live)))
    ]
    for load in loads:
        load.start()
    for l in range(layers):
        pltpu.make_async_copy(weight_hbm.at[l, 0], w.at[l], wsem.at[l]).start()
    barrier = pltpu.get_barrier_semaphore()
    for a, b, own in peers:
        if not own:
            pl.semaphore_signal(barrier, inc=1, device_id=at(a, b), device_id_type=MESH)

    for load in loads:
        load.wait()
    for j in range(nd):
        for r in range(width):
            s = (j * width + r) * block
            fsend[j, r] = feat[:, s:s + block]
    lane = lax.broadcasted_iota(jnp.int32, (1, block), 1)
    auxs[...] = jnp.zeros_like(auxs)
    for r in range(width):
        auxs[r:r + 1, :] = bias[layers - 1:layers, r * block:(r + 1) * block]
    for l in range(layers):
        cols = jnp.zeros((1, block), jnp.int32)
        for s in range(nd):
            cols = jnp.where(lane == s, col[l, 0, s], cols)
        auxs[width + l:width + l + 1, :] = cols.astype(f32)
    pl.semaphore_wait(barrier, nd - 1)

    pending = []

    def send(src, dst, send_sem, recv_sem, a, b, own):
        if own:
            pltpu.make_async_copy(src, dst, recv_sem).start()
        else:
            c = pltpu.make_async_remote_copy(src, dst, send_sem, recv_sem, device_id=at(a, b), device_id_type=MESH)
            c.start()
            pending.append(c)

    def arrived(ref, sem):
        pltpu.make_async_copy(ref, ref, sem).wait()

    for k, (a, b, own) in enumerate(peers):
        send(fsend.at[a * ny + b], fin.at[my_place], fs.at[k], fr.at[my_place], a, b, own)
    for k, (a, b, own) in enumerate(peers):
        send(auxs, aux.at[me], xs.at[k], xr.at[me], a, b, own)

    def product(l, c, e):
        x = act[row[l, 0, e], c * half:(c + 1) * half, :]
        t = jnp.dot(x, w[l, e], preferred_element_type=f32)
        return (t * live[l, 0, e].astype(f32)).astype(jnp.bfloat16)

    far_z, relay_z = (1 - hi) * hz, hi + hz - 1
    relay = my_z == relay_z
    slot = my_x * hz + lo
    guarded = []

    def source(n):
        return (n // hz) * ny + hi * hz + n % hz

    def send_terms(l, c):
        order = list(range(1, nx)) + [0]
        for k, i in enumerate(order):
            for n in range(hz):
                rsend[l, c, k, n] = product(l, c, (my_x + i) % nx * ny + far_z + n)
        for k, i in enumerate(order):
            a = (my_x + i) % nx
            src, dst = rsend.at[l, c, k], rrecv.at[l, c, slot]
            cp = pltpu.make_async_remote_copy(
                src, dst, rs.at[l, c, k], rr.at[l, c, slot], device_id=at(a, relay_z), device_id_type=MESH
            )
            if i == 0:
                @pl.when(relay)
                def _():
                    pltpu.make_async_copy(src, dst, rr.at[l, c, slot]).start()

                @pl.when(jnp.logical_not(relay))
                def _():
                    cp.start()
                guarded.append((jnp.logical_not(relay), cp))
            else:
                cp.start()
                pending.append(cp)
        steps = [(n, i) for n in list(range(1, hz)) + [0] for i in order]
        for k, (n, i) in enumerate(steps):
            tsend[l, c, k] = product(l, c, (my_x + i) % nx * ny + hi * hz + (lo + n) % hz)
        k = 0
        for n in list(range(1, hz)) + [0]:
            b = hi * hz + (lo + n) % hz
            for i in list(range(1, nx)) + [0]:
                a = (my_x + i) % nx
                send(tsend.at[l, c, k], trecv.at[l, c, slot], ts.at[l, c, k], tr.at[l, c, slot], a, b, n == 0 and i == 0)
                k += 1

    def forward(l, c):
        rows_of = [[(l * hz + i) * nd + source(n) for n in range(nx * hz)] for i in range(hz)]
        cps = [
            pltpu.make_async_remote_copy(
                psend.at[l, c, i], precv.at[l, c], ps.at[l, c, i], pr.at[l, c],
                device_id=at(my_x, far_z + i), device_id_type=MESH
            )
            for i in range(hz)
        ]

        @pl.when(relay)
        def _():
            for n in range(nx * hz):
                arrived(rrecv.at[l, c, n], rr.at[l, c, n])
            for i in range(hz):
                for t0 in range(0, half, 32):
                    acc = [jnp.zeros((32, block), f32) for q in range(width)]
                    for n in range(nx * hz):
                        t = rrecv[l, c, n, i, t0:t0 + 32, :].astype(f32)
                        v = colr[pl.ds(rows_of[i][n], 1)][0]
                        v = jnp.concatenate([v] * 4, axis=0)
                        for q in range(width):
                            acc[q] = acc[q] + jnp.where(v == float(q), t, 0.0)
                    for q in range(width):
                        psend[l, c, i, q, t0:t0 + 32, :] = acc[q].astype(jnp.bfloat16)
                cps[i].start()
        guarded.extend((relay, cp) for cp in cps)

    def send_last(c):
        l = layers - 1
        for e in range(nd):
            t = product(l, c, e).astype(f32).reshape(per, rows, block)
            osend[c * per:(c + 1) * per, e] = t.astype(jnp.bfloat16)
        core, far = my_x % CHUNKS, my_x // CHUNKS
        groups = nx // CHUNKS
        k = 0
        for n, b in enumerate(zs):
            for i in list(range(1, groups)) + [0]:
                a = ((far + i) % groups) * CHUNKS + c
                src, dst = osend.at[place(a, b)], orecv.at[me]
                cp = pltpu.make_async_remote_copy(src, dst, os.at[c, k], orr.at[me], device_id=at(a, b), device_id_type=MESH)
                k += 1
                if i == 0 and n == ny - 1:
                    @pl.when(core == c)
                    def _():
                        pltpu.make_async_copy(src, dst, orr.at[me]).start()

                    @pl.when(core != c)
                    def _():
                        cp.start()
                    lasts.append((c, cp))
                else:
                    cp.start()
                    pending.append(cp)

    lasts = []

    for c in range(CHUNKS):
        for p in range(c * per, (c + 1) * per):
            arrived(fin.at[p], fr.at[p])
        for r in range(width):
            x = fin[c * per:(c + 1) * per, r].astype(f32).reshape(half, block)
            act[r, c * half:(c + 1) * half, :] = x.astype(jnp.bfloat16)
        if c == 0:
            arrived(w.at[0], wsem.at[0])
        send_terms(0, c)

    for g in range(nd):
        arrived(aux.at[g], xr.at[g])
    eye = lax.broadcasted_iota(jnp.int32, (nd, block), 0) == lax.broadcasted_iota(jnp.int32, (nd, block), 1)
    ones = jnp.ones((block, block), jnp.bfloat16)
    for e in range(nd):
        last = width + layers - 1
        v = jnp.where(eye, aux[e, last:last + 1, :], 0.0).astype(jnp.bfloat16)
        colx[e * nd:(e + 1) * nd, :] = jnp.dot(v, ones, preferred_element_type=f32)

    for l in range(layers - 1):
        for i in range(hz):
            v = jnp.where(eye, aux[my_x * ny + far_z + i, width + l:width + l + 1, :], 0.0).astype(jnp.bfloat16)
            m = jnp.dot(v, ones, preferred_element_type=f32)
            k = (l * hz + i) * nd
            colr[k:k + nd] = jnp.broadcast_to(m[:, None, :], (nd, 8, block))
    for c in range(CHUNKS):
        forward(0, c)

    tile = 32
    for l in range(1, layers):
        arrived(w.at[l], wsem.at[l])
        for c in range(CHUNKS):
            for n in range(nx * hz):
                arrived(trecv.at[l - 1, c, n], tr.at[l - 1, c, n])
            arrived(precv.at[l - 1, c], pr.at[l - 1, c])
            for t0 in range(0, half, tile):
                acc = [jnp.broadcast_to(bias[l - 1:l, q * block:(q + 1) * block], (tile, block)) for q in range(width)]
                acc = [acc[q] + precv[l - 1, c, q, t0:t0 + tile, :].astype(f32) for q in range(width)]
                for n in range(nx * hz):
                    t = trecv[l - 1, c, n, t0:t0 + tile, :].astype(f32)
                    where = col[l - 1, 0, source(n)]
                    for q in range(width):
                        acc[q] = acc[q] + t * (where == q).astype(f32)
                for q in range(width):
                    act[q, c * half + t0:c * half + t0 + tile, :] = jnp.maximum(acc[q], 0.0).astype(jnp.bfloat16)
            if l < layers - 1:
                send_terms(l, c)
            else:
                send_last(c)
        if l < layers - 1:
            for c in range(CHUNKS):
                forward(l, c)

    for g in range(nd):
        arrived(orecv.at[g], orr.at[g])
    for e in range(nd):
        acc = [jnp.broadcast_to(aux[e, q:q + 1, :], (rows, block)) for q in range(width)]
        for g in range(nd):
            t = orecv[g, e].astype(f32)
            where = jnp.broadcast_to(colx[e * nd + g:e * nd + g + 1, :], (rows, block))
            for q in range(width):
                acc[q] = acc[q] + jnp.where(where == float(q), t, 0.0)
        for q in range(width):
            s = (e * width + q) * block
            out[:, s:s + block] = jnp.maximum(acc[q], 0.0).astype(jnp.bfloat16)

    for cp in pending:
        cp.wait_send()
    for started, cp in guarded:
        @pl.when(started)
        def _():
            cp.wait_send()
    for c, cp in lasts:
        @pl.when(my_x % CHUNKS != c)
        def _():
            cp.wait_send()


def fused(nx, ny, features, link_weight, link_row, link_col, link_live, bias):
    nd = nx * ny
    layers = bias.shape[0]
    block = link_weight.shape[-1]
    width = bias.shape[1] // block
    rows = features.shape[0]
    half = rows * nd // CHUNKS
    hz = ny // 2
    bf16 = jnp.bfloat16
    vmem = pl.BlockSpec(memory_space=pltpu.VMEM)
    counts = pltpu.SMEM((layers, 1, nd), jnp.int32)
    dma = pltpu.SemaphoreType.DMA
    return pl.pallas_call(
        functools.partial(kernel, nx, ny),
        out_shape=pltpu.VMEM(features.shape, bf16),
        in_specs=[pl.BlockSpec(memory_space=pl.ANY)] * 6,
        out_specs=vmem,
        scratch_shapes=[
            pltpu.VMEM(features.shape, bf16),
            counts, counts, counts,
            pltpu.VMEM(bias.shape, jnp.float32),
            dma((5,)),
            pltpu.VMEM((layers, nd, block, block), bf16),
            pltpu.VMEM((nd, width, rows, block), bf16),
            pltpu.VMEM((nd, width, rows, block), bf16),
            pltpu.VMEM((width, rows * nd, block), bf16),
            pltpu.VMEM((layers - 1, CHUNKS, nx * hz, half, block), bf16),
            pltpu.VMEM((layers - 1, CHUNKS, nx * hz, half, block), bf16),
            pltpu.VMEM((nd, nd, rows, block), bf16),
            pltpu.VMEM((nd, nd, rows, block), bf16),
            pltpu.VMEM((nd, 8, block), jnp.float32),
            pltpu.VMEM((8, block), jnp.float32),
            pltpu.VMEM((nd * nd, block), jnp.float32),
            pltpu.VMEM((layers - 1, CHUNKS, nx, hz, half, block), bf16),
            pltpu.VMEM((layers - 1, CHUNKS, nx * hz, hz, half, block), bf16),
            pltpu.VMEM((layers - 1, CHUNKS, hz, width, half, block), bf16),
            pltpu.VMEM((layers - 1, CHUNKS, width, half, block), bf16),
            pltpu.VMEM(((layers - 1) * hz * nd, 8, block), jnp.float32),
            dma((layers,)),
            dma((nd,)), dma((nd,)), dma((nd,)), dma((nd,)),
            dma((layers - 1, CHUNKS, nx * hz)), dma((layers - 1, CHUNKS, nx * hz)),
            dma((CHUNKS, nd)), dma((nd,)),
            dma((layers - 1, CHUNKS, nx)), dma((layers - 1, CHUNKS, nx * hz)),
            dma((layers - 1, CHUNKS, hz)), dma((layers - 1, CHUNKS)),
        ],
        compiler_params=pltpu.CompilerParams(
            collective_id=0, has_side_effects=True, vmem_limit_bytes=60 * 1024 * 1024
        ),
    )(features, link_weight, link_row, jnp.transpose(link_col, (0, 2, 1)), link_live, bias)


def solution(mesh):
    placed = (
        P(("nx", "ny", "img"), None),
        P(None, ("nx", "ny"), None, None, None),
        P(None, ("nx", "ny"), None),
        P(None, None, ("nx", "ny")),
        P(None, ("nx", "ny"), None),
        P(None, ("nx", "ny")),
    )
    nx, ny = mesh.shape["nx"], mesh.shape["ny"]

    def run(features, link_weight, link_row, link_col, link_live, bias):
        block = link_weight.shape[-1]
        rows = features.shape[0]
        width = bias.shape[1] // block
        fits = (
            rows % 8 == 0 and nx % CHUNKS == 0 and ny % 2 == 0 and block == 128
            and nx * ny <= 32 and width + bias.shape[0] <= 8 and (rows * nx * ny) % (32 * CHUNKS) == 0 and bias.shape[0] > 1
        )
        step = functools.partial(fused, nx, ny) if fits else local
        return step(features, link_weight, link_row, link_col, link_live, bias)

    return jax.shard_map(
        run, mesh=mesh, in_specs=placed, out_specs=P(("nx", "ny", "img"), None), check_vma=False
    )
```

```python
import functools

import jax
import jax.numpy as jnp
from jax import lax
from jax.experimental import pallas as pl
from jax.experimental.pallas import tpu as pltpu
from jax.sharding import PartitionSpec as P

MESH = pl.DeviceIdType.MESH
LAG = 2


def combine_links(received, col_ids, width):
    onehot = (col_ids[:, None] == jnp.arange(width, dtype=jnp.int32)[None, :]).astype(jnp.bfloat16)
    summed = jnp.einsum("dq,dis->iqs", onehot, received, preferred_element_type=jnp.float32)
    return summed.reshape(summed.shape[0], width * received.shape[2])


def link_products(blocks, weights, row_ids, live_mask):
    masked = weights * live_mask.astype(jnp.bfloat16)[:, None, None]
    gathered = jnp.take(blocks, row_ids, axis=1)
    result = jnp.einsum(
        "ier,ers->eis", gathered, masked, preferred_element_type=jnp.float32
    ).astype(jnp.bfloat16)
    return result


def local(features, link_weight, link_row, link_col, link_live, bias):
    block_size = link_weight.shape[-1]
    width = bias.shape[1] // block_size
    hidden = lax.all_to_all(features, ("nx", "ny"), split_axis=1, concat_axis=0, tiled=True)
    image_rows = hidden.shape[0]
    for layer_idx in range(bias.shape[0]):
        blocks = hidden.reshape(image_rows, width, block_size)
        link_terms = link_products(
            blocks, link_weight[layer_idx, 0], link_row[layer_idx, 0], link_live[layer_idx, 0]
        )
        col_ids = link_col[layer_idx, :, 0]
        summed = combine_links(
            lax.all_to_all(link_terms, ("nx", "ny"), split_axis=0, concat_axis=0, tiled=True),
            col_ids,
            width,
        )
        hidden = jnp.maximum(summed + bias[layer_idx][None, :], 0.0).astype(jnp.bfloat16)
    finished = lax.all_to_all(hidden, ("nx", "ny"), split_axis=0, concat_axis=1, tiled=True)
    return finished


def kernel(nx, ny, feat_hbm, weight_hbm, row_hbm, col_hbm, live_hbm, bias_hbm, out, feat, row, col, live, bias, isem, w, wsem,
           fin, fs, fr, act, auxs, aux, xs, xr, colx, colr, tsend, trecv, ts, tr, rsend, rrecv, rs, ro, rr, psend, precv, ps, pr,
           lsend, orecv, ls, orr, qrecv, qr, usend, urecv, us, ur, pre):
    nd = nx * ny
    layers = bias.shape[0]
    block = w.shape[-1]
    width = bias.shape[1] // block
    rows = feat.shape[0]
    hz = ny // 2
    chunks = 2 * hz
    per = nd // chunks
    size = per * rows
    near = nx * hz
    f32, bf16 = jnp.float32, jnp.bfloat16
    my_x, my_z = lax.axis_index("nx"), lax.axis_index("ny")
    me = my_x * ny + my_z
    hi, lo = my_z // hz, my_z % hz
    far_z, relay_z = (1 - hi) * hz, hi + hz - 1
    relay = my_z == relay_z
    slot = my_x * hz + lo

    zs = [(1 - hi) * hz + (lo + i) % hz for i in range(hz)] + [hi * hz + (lo + i) % hz for i in range(1, hz)] + [my_z]
    peers = [((my_x + i) % nx, z, i == 0 and n == ny - 1) for n, z in enumerate(zs) for i in list(range(1, nx)) + [0]]

    def place(a, b):
        return ((a % 2) * hz + b % hz) * per + (a // 2) * 2 + b // hz

    def remote(src, dst, send_sem, recv_sem, a, b):
        return pltpu.make_async_remote_copy(src, dst, send_sem, recv_sem, device_id={"nx": a, "ny": b}, device_id_type=MESH)

    def send(src, dst, send_sem, recv_sem, a, b, own):
        if own:
            pltpu.make_async_copy(src, dst, recv_sem).start()
        else:
            remote(src, dst, send_sem, recv_sem, a, b).start()

    def arrived(ref, sem):
        pltpu.make_async_copy(ref, ref, sem).wait()

    loads = [
        pltpu.make_async_copy(src, dst, isem.at[n])
        for n, (src, dst) in enumerate(((feat_hbm, feat), (bias_hbm, bias), (col_hbm, col), (row_hbm, row), (live_hbm, live)))
    ]
    for load in loads:
        load.start()
    for l in range(layers):
        pltpu.make_async_copy(weight_hbm.at[l, 0], w.at[l], wsem.at[l]).start()
    barrier = pltpu.get_barrier_semaphore()
    for a, b, own in peers:
        if not own:
            pl.semaphore_signal(barrier, inc=1, device_id={"nx": a, "ny": b}, device_id_type=MESH)

    for load in loads:
        load.wait()
    lane = lax.broadcasted_iota(jnp.int32, (1, block), 1)
    auxs[...] = jnp.zeros_like(auxs)
    for r in range(width):
        auxs[r:r + 1, :] = bias[layers - 1:layers, r * block:(r + 1) * block]
    for l in range(layers):
        cols = jnp.zeros((1, block), jnp.int32)
        for s in range(nd):
            cols = jnp.where(lane == s, col[l, 0, s], cols)
        auxs[width + l:width + l + 1, :] = cols.astype(f32)
    pl.semaphore_wait(barrier, nd - 1)

    my_place = place(my_x, my_z)
    my_chunk = my_place // per
    span = width * block
    for a, b, own in peers:
        at = pl.multiple_of((a * ny + b) * span, span)
        send(feat.at[:, pl.ds(at, span)], fin.at[my_place], fs, fr.at[my_chunk], a, b, own)
    for a, b, own in peers:
        send(auxs, aux.at[me], xs, xr, a, b, own)

    def product(l, c, e):
        x = act[row[l, 0, e], c * size:(c + 1) * size, :]
        t = jnp.dot(x, w[l, e], preferred_element_type=f32)
        return t * live[l, 0, e].astype(f32)

    def source(n):
        return (n // hz) * ny + hi * hz + n % hz

    order = list(range(1, nx)) + [0]
    steps = [(n, i) for n in list(range(1, hz)) + [0] for i in order]

    def send_terms(l, c):
        k = l * chunks + c
        for j, i in enumerate(order):
            for n in range(hz):
                rsend[j, k, n] = product(l, c, (my_x + i) % nx * ny + far_z + n).astype(bf16)
        for j, i in enumerate(order):
            a = (my_x + i) % nx
            src, dst = rsend.at[j, k], rrecv.at[k, slot]
            if i == 0:
                @pl.when(relay)
                def _():
                    pltpu.make_async_copy(src, dst, rr.at[k]).start()

                @pl.when(jnp.logical_not(relay))
                def _():
                    remote(src, dst, ro, rr.at[k], a, relay_z).start()
            else:
                remote(src, dst, rs, rr.at[k], a, relay_z).start()
        for j, (n, i) in enumerate(steps):
            tsend[j, k] = product(l, c, (my_x + i) % nx * ny + hi * hz + (lo + n) % hz).astype(bf16)
        for j, (n, i) in enumerate(steps):
            a, b = (my_x + i) % nx, hi * hz + (lo + n) % hz
            send(tsend.at[j, k], trecv.at[k, slot], ts, tr.at[k], a, b, n == 0 and i == 0)

    def forward(l, c):
        k = l * chunks + c

        @pl.when(relay)
        def _():
            arrived(rrecv.at[k], rr.at[k])
            for i in range(hz):
                acc = [jnp.zeros((size, block), f32) for q in range(width)]
                for n in range(near):
                    t = rrecv[k, n, i].astype(f32)
                    v = colr[pl.ds((l * hz + i) * nd + source(n), 1)][0]
                    v = jnp.concatenate([v] * (size // 8), axis=0)
                    for q in range(width):
                        acc[q] = acc[q] + jnp.where(v == float(q), t, 0.0)
                for q in range(width):
                    psend[k, i, q] = acc[q].astype(bf16)
                remote(psend.at[k, i], precv.at[k], ps, pr.at[k], my_x, far_z + i).start()

    def collect(l, c):
        k = l * chunks + c
        arrived(trecv.at[k], tr.at[k])
        arrived(precv.at[k], pr.at[k])
        acc = [jnp.broadcast_to(bias[l:l + 1, q * block:(q + 1) * block], (size, block)) for q in range(width)]
        acc = [acc[q] + precv[k, q].astype(f32) for q in range(width)]
        for n in range(near):
            t = trecv[k, n].astype(f32)
            where = col[l, 0, source(n)]
            for q in range(width):
                acc[q] = acc[q] + t * (where == q).astype(f32)
        for q in range(width):
            act[q, c * size:(c + 1) * size, :] = jnp.maximum(acc[q], 0.0).astype(bf16)

    def owners(c):
        p, q = c // hz, c % hz
        return [(2 * j + p, (1 - hi) * hz + q, 2 * j + 1 - hi) for j in range(nx // 2)], [
            (2 * j + p, hi * hz + q, 2 * j + hi) for j in range(nx // 2)]

    def send_last(c):
        l = layers - 1
        p, q = c // hz, c % hz
        far, close = owners(c)
        for e in range(nd):
            t = product(l, c, e).reshape(per, rows, block)
            lsend[c * per:(c + 1) * per, e] = t.astype(bf16)
        for a, b, o in far:
            src, dst = lsend.at[c * per + o], qrecv.at[q, slot]
            mine = jnp.logical_and(relay, my_x == a)

            @pl.when(mine)
            def _():
                pltpu.make_async_copy(src, dst, qr.at[q]).start()

            @pl.when(jnp.logical_not(mine))
            def _():
                remote(src, dst, ls, qr.at[q], a, relay_z).start()
        for a, b, o in close:
            src, dst = lsend.at[c * per + o], orecv.at[slot]
            mine = jnp.logical_and(my_z == b, my_x == a)

            @pl.when(mine)
            def _():
                pltpu.make_async_copy(src, dst, orr).start()

            @pl.when(jnp.logical_not(mine))
            def _():
                remote(src, dst, ls, orr, a, b).start()

    def forward_last(c):
        p, q = c // hz, c % hz

        @pl.when(jnp.logical_and(relay, my_x % 2 == p))
        def _():
            arrived(qrecv.at[q], qr.at[q])
            for e in range(nd):
                acc = [jnp.zeros((rows, block), f32) for r in range(width)]
                for n in range(near):
                    t = qrecv[q, n, e].astype(f32)
                    v = jnp.broadcast_to(colx[pl.ds(e * nd + source(n), 1), :], (rows, block))
                    for r in range(width):
                        acc[r] = acc[r] + jnp.where(v == float(r), t, 0.0)
                for r in range(width):
                    usend[q, e, r] = acc[r].astype(bf16)
            remote(usend.at[q], urecv, us, ur, my_x, far_z + q).start()

    for c in range(chunks):
        arrived(fin.at[c * per:(c + 1) * per], fr.at[c])
        for r in range(width):
            x = fin[c * per:(c + 1) * per, :, r * block:(r + 1) * block].astype(f32).reshape(size, block)
            act[r, c * size:(c + 1) * size, :] = x.astype(bf16)
        if c == 0:
            arrived(w.at[0], wsem.at[0])
        send_terms(0, c)

    arrived(aux, xr)
    eye = lax.broadcasted_iota(jnp.int32, (nd, block), 0) == lax.broadcasted_iota(jnp.int32, (nd, block), 1)
    ones = jnp.ones((block, block), bf16)
    for l in range(layers - 1):
        for i in range(hz):
            v = jnp.where(eye, aux[my_x * ny + far_z + i, width + l:width + l + 1, :], 0.0).astype(bf16)
            m = jnp.dot(v, ones, preferred_element_type=f32)
            k = (l * hz + i) * nd
            colr[k:k + nd] = jnp.broadcast_to(m[:, None, :], (nd, 8, block))
    for e in range(nd):
        last = width + layers - 1
        v = jnp.where(eye, aux[e, last:last + 1, :], 0.0).astype(bf16)
        colx[e * nd:(e + 1) * nd, :] = jnp.dot(v, ones, preferred_element_type=f32)

    total = layers * chunks

    def relay_step(k):
        if k < total - chunks:
            forward(k // chunks, k % chunks)
        elif k < total:
            forward_last(k % chunks)

    for k in range(LAG):
        relay_step(k)
    for k in range(total - chunks):
        relay_step(k + LAG)
        l, c = k // chunks, k % chunks
        collect(l, c)
        if c == 0:
            arrived(w.at[l + 1], wsem.at[l + 1])
        if l + 1 < layers - 1:
            send_terms(l + 1, c)
        else:
            send_last(c)
    for k in range(total - chunks + LAG, total):
        relay_step(k)

    arrived(orecv, orr)
    for e in range(nd):
        acc = [jnp.broadcast_to(aux[e, q:q + 1, :], (rows, block)) for q in range(width)]
        for n in range(near):
            t = orecv[n, e].astype(f32)
            v = jnp.broadcast_to(colx[pl.ds(e * nd + source(n), 1), :], (rows, block))
            for q in range(width):
                acc[q] = acc[q] + jnp.where(v == float(q), t, 0.0)
        for q in range(width):
            pre[e * width + q] = acc[q]
    arrived(urecv, ur)
    for e in range(nd):
        for q in range(width):
            s = (e * width + q) * block
            out[:, s:s + block] = jnp.maximum(pre[e * width + q] + urecv[e, q].astype(f32), 0.0).astype(bf16)

    arrived(fin.at[0:nd - 1], fs)
    arrived(aux.at[0:nd - 1], xs)
    arrived(tsend.at[0:near - 1], ts)
    arrived(rsend.at[0:nx - 1], rs)

    @pl.when(relay)
    def _():
        arrived(psend, ps)
        arrived(usend, us)
        arrived(lsend.at[0:nd - 1 - hz], ls)

    @pl.when(jnp.logical_not(relay))
    def _():
        arrived(rsend.at[nx - 1], ro)
        arrived(lsend.at[0:nd - 1], ls)


def fused(nx, ny, features, link_weight, link_row, link_col, link_live, bias):
    nd = nx * ny
    layers = bias.shape[0]
    block = link_weight.shape[-1]
    width = bias.shape[1] // block
    rows = features.shape[0]
    hz = ny // 2
    chunks = 2 * hz
    per = nd // chunks
    size = per * rows
    near = nx * hz
    steps = (layers - 1) * chunks
    bf16, f32 = jnp.bfloat16, jnp.float32
    vmem = pltpu.VMEM
    counts = pltpu.SMEM((layers, 1, nd), jnp.int32)
    dma = pltpu.SemaphoreType.DMA
    return pl.pallas_call(
        functools.partial(kernel, nx, ny),
        out_shape=vmem(features.shape, bf16),
        in_specs=[pl.BlockSpec(memory_space=pl.ANY)] * 6,
        out_specs=pl.BlockSpec(memory_space=vmem),
        scratch_shapes=[
            vmem(features.shape, bf16), counts, counts, counts, vmem(bias.shape, f32), dma((5,)),
            vmem((layers, nd, block, block), bf16), dma((layers,)),
            vmem((nd, rows, width * block), bf16), dma, dma((chunks,)),
            vmem((width, rows * nd, block), bf16),
            vmem((8, block), f32), vmem((nd, 8, block), f32), dma, dma,
            vmem((nd * nd, block), f32), vmem(((layers - 1) * hz * nd, 8, block), f32),
            vmem((near, steps, size, block), bf16), vmem((steps, near, size, block), bf16), dma, dma((steps,)),
            vmem((nx, steps, hz, size, block), bf16), vmem((steps, near, hz, size, block), bf16), dma, dma, dma((steps,)),
            vmem((steps, hz, width, size, block), bf16), vmem((steps, width, size, block), bf16), dma, dma((steps,)),
            vmem((nd, nd, rows, block), bf16), vmem((near, nd, rows, block), bf16), dma, dma,
            vmem((hz, near, nd, rows, block), bf16), dma((hz,)),
            vmem((hz, nd, width, rows, block), bf16), vmem((nd, width, rows, block), bf16), dma, dma,
            vmem((nd * width, rows, block), f32),
        ],
        compiler_params=pltpu.CompilerParams(
            collective_id=0, has_side_effects=True, vmem_limit_bytes=60 * 1024 * 1024
        ),
    )(features, link_weight, link_row, jnp.transpose(link_col, (0, 2, 1)), link_live, bias)


def solution(mesh):
    placed = (
        P(("nx", "ny", "img"), None),
        P(None, ("nx", "ny"), None, None, None),
        P(None, ("nx", "ny"), None),
        P(None, None, ("nx", "ny")),
        P(None, ("nx", "ny"), None),
        P(None, ("nx", "ny")),
    )
    nx, ny = mesh.shape["nx"], mesh.shape["ny"]

    def run(features, link_weight, link_row, link_col, link_live, bias):
        block = link_weight.shape[-1]
        rows = features.shape[0]
        width = bias.shape[1] // block
        fits = (
            rows % 8 == 0 and nx % 2 == 0 and ny % 2 == 0 and block == 128
            and nx * ny <= 32 and width + bias.shape[0] <= 8 and (nx * rows) % 16 == 0 and bias.shape[0] > 1
        )
        step = functools.partial(fused, nx, ny) if fits else local
        return step(features, link_weight, link_row, link_col, link_live, bias)

    return jax.shard_map(
        run, mesh=mesh, in_specs=placed, out_specs=P(("nx", "ny", "img"), None), check_vma=False
    )
```

```python
import functools

import jax
import jax.numpy as jnp
from jax import lax
from jax.experimental import pallas as pl
from jax.experimental.pallas import tpu as pltpu
from jax.sharding import PartitionSpec as P

MESH = pl.DeviceIdType.MESH
LAG = 2
GROUPS = 4
DEPTH = 1
DEPTH_LAST = 1


def combine_links(received, col_ids, width):
    onehot = (col_ids[:, None] == jnp.arange(width, dtype=jnp.int32)[None, :]).astype(jnp.bfloat16)
    summed = jnp.einsum("dq,dis->iqs", onehot, received, preferred_element_type=jnp.float32)
    return summed.reshape(summed.shape[0], width * received.shape[2])


def link_products(blocks, weights, row_ids, live_mask):
    masked = weights * live_mask.astype(jnp.bfloat16)[:, None, None]
    gathered = jnp.take(blocks, row_ids, axis=1)
    result = jnp.einsum(
        "ier,ers->eis", gathered, masked, preferred_element_type=jnp.float32
    ).astype(jnp.bfloat16)
    return result


def local(features, link_weight, link_row, link_col, link_live, bias):
    block_size = link_weight.shape[-1]
    width = bias.shape[1] // block_size
    hidden = lax.all_to_all(features, ("nx", "ny"), split_axis=1, concat_axis=0, tiled=True)
    image_rows = hidden.shape[0]
    for layer_idx in range(bias.shape[0]):
        blocks = hidden.reshape(image_rows, width, block_size)
        link_terms = link_products(
            blocks, link_weight[layer_idx, 0], link_row[layer_idx, 0], link_live[layer_idx, 0]
        )
        col_ids = link_col[layer_idx, :, 0]
        summed = combine_links(
            lax.all_to_all(link_terms, ("nx", "ny"), split_axis=0, concat_axis=0, tiled=True),
            col_ids,
            width,
        )
        hidden = jnp.maximum(summed + bias[layer_idx][None, :], 0.0).astype(jnp.bfloat16)
    finished = lax.all_to_all(hidden, ("nx", "ny"), split_axis=0, concat_axis=1, tiled=True)
    return finished


def kernel(nx, ny, feat_hbm, weight_hbm, row_hbm, col_hbm, live_hbm, bias_hbm, out, feat, row, col, live, bias, isem, w, wsem,
           fin, fs, fr, act, auxs, aux, xs, xr, colx, colr, tsend, trecv, ts, tr, rsend, rrecv, rs, ro, rr, psend, precv, ps, pr,
           lsend, orecv, ls, orr, qrecv, qr, usend, urecv, us, ur, pre):
    nd = nx * ny
    layers = bias.shape[0]
    block = w.shape[-1]
    width = bias.shape[1] // block
    rows = feat.shape[0]
    hz = ny // 2
    chunks = 2 * hz
    per = nd // chunks
    size = per * rows
    near = nx * hz
    f32, bf16 = jnp.float32, jnp.bfloat16
    part = nd // GROUPS
    my_x, my_z = lax.axis_index("nx"), lax.axis_index("ny")
    me = my_x * ny + my_z
    hi, lo = my_z // hz, my_z % hz
    far_z, relay_z = (1 - hi) * hz, hi + hz - 1
    relay = my_z == relay_z
    slot = my_x * hz + lo

    zs = [hi * i + (1 - hi) * (ny - 1 - i) for i in range(hz)] + [hi * hz + (lo + i) % hz for i in range(1, hz)] + [my_z]
    peers = [((my_x + i) % nx, z, i == 0 and n == ny - 1) for n, z in enumerate(zs) for i in list(range(1, nx)) + [0]]

    def place(a, b):
        d = (b // hz) * (b - hz) + (1 - b // hz) * (hz - 1 - b)
        p = a % 2
        return (p * hz + (1 - p) * d + p * (hz - 1 - d)) * per + (a // 2) * 2 + b // hz

    def remote(src, dst, send_sem, recv_sem, a, b):
        return pltpu.make_async_remote_copy(src, dst, send_sem, recv_sem, device_id={"nx": a, "ny": b}, device_id_type=MESH)

    def send(src, dst, send_sem, recv_sem, a, b, own):
        if own:
            pltpu.make_async_copy(src, dst, recv_sem).start()
        else:
            remote(src, dst, send_sem, recv_sem, a, b).start()

    def arrived(ref, sem):
        pltpu.make_async_copy(ref, ref, sem).wait()

    loads = [
        pltpu.make_async_copy(src, dst, isem.at[n])
        for n, (src, dst) in enumerate(((feat_hbm, feat), (bias_hbm, bias), (col_hbm, col), (row_hbm, row), (live_hbm, live)))
    ]
    for load in loads:
        load.start()
    for l in range(layers):
        pltpu.make_async_copy(weight_hbm.at[l, 0], w.at[l], wsem.at[l]).start()
    barrier = pltpu.get_barrier_semaphore()
    for a, b, own in peers:
        if not own:
            pl.semaphore_signal(barrier, inc=1, device_id={"nx": a, "ny": b}, device_id_type=MESH)

    for load in loads:
        load.wait()
    lane = lax.broadcasted_iota(jnp.int32, (1, block), 1)
    auxs[...] = jnp.zeros_like(auxs)
    for r in range(width):
        auxs[r:r + 1, :] = bias[layers - 1:layers, r * block:(r + 1) * block]
    for l in range(layers):
        cols = jnp.zeros((1, block), jnp.int32)
        for s in range(nd):
            cols = jnp.where(lane == s, col[l, 0, s], cols)
        auxs[width + l:width + l + 1, :] = cols.astype(f32)
    pl.semaphore_wait(barrier, nd - 1)

    my_place = place(my_x, my_z)
    my_chunk = my_place // per
    span = width * block
    for a, b, own in peers:
        at = pl.multiple_of((a * ny + b) * span, span)
        send(feat.at[:, pl.ds(at, span)], fin.at[my_place], fs, fr.at[my_chunk], a, b, own)
    for a, b, own in peers:
        send(auxs, aux.at[me], xs, xr, a, b, own)

    def product(l, c, e):
        x = act[row[l, 0, e], c * size:(c + 1) * size, :]
        t = jnp.dot(x, w[l, e], preferred_element_type=f32)
        return t * live[l, 0, e].astype(f32)

    def source(n):
        return (n // hz) * ny + hi * hz + n % hz

    order = list(range(1, nx)) + [0]
    steps = [(n, i) for n in list(range(1, hz)) + [0] for i in order]

    held = []

    def release(depth):
        while len(held) > depth:
            for start in held.pop(0):
                start()

    def send_bundle(l, c, j, i):
        k = l * chunks + c
        a = (my_x + i) % nx
        src, dst = rsend.at[j, k], rrecv.at[k, slot]
        if i == 0:
            @pl.when(relay)
            def _():
                pltpu.make_async_copy(src, dst, rr.at[k]).start()

            @pl.when(jnp.logical_not(relay))
            def _():
                remote(src, dst, ro, rr.at[k], a, relay_z).start()
        else:
            remote(src, dst, rs, rr.at[k], a, relay_z).start()

    def send_near(k, j, n, i):
        a, b = (my_x + i) % nx, hi * hz + (lo + n) % hz
        send(tsend.at[j, k], trecv.at[k, slot], ts, tr.at[k], a, b, n == 0 and i == 0)

    def send_terms(l, c):
        k = l * chunks + c
        for j, i in enumerate(order):
            for n in range(hz):
                rsend[j, k, n] = product(l, c, (my_x + i) % nx * ny + far_z + n).astype(bf16)
        for j, i in enumerate(order):
            send_bundle(l, c, j, i)
        release(DEPTH - 1)
        for j, (n, i) in enumerate(steps):
            tsend[j, k] = product(l, c, (my_x + i) % nx * ny + hi * hz + (lo + n) % hz).astype(bf16)
        held.append([functools.partial(send_near, k, j, n, i) for j, (n, i) in enumerate(steps)])

    def forward(l, c):
        k = l * chunks + c

        @pl.when(relay)
        def _():
            arrived(rrecv.at[k], rr.at[k])
            for i in range(hz):
                acc = [jnp.zeros((size, block), f32) for q in range(width)]
                for n in range(near):
                    t = rrecv[k, n, i].astype(f32)
                    v = colr[pl.ds((l * hz + i) * nd + source(n), 1)][0]
                    v = jnp.concatenate([v] * (size // 8), axis=0)
                    for q in range(width):
                        acc[q] = acc[q] + jnp.where(v == float(q), t, 0.0)
                for q in range(width):
                    psend[k, i, q] = acc[q].astype(bf16)
                remote(psend.at[k, i], precv.at[k], ps, pr.at[k], my_x, far_z + i).start()

    def collect(l, c):
        k = l * chunks + c
        arrived(trecv.at[k], tr.at[k])
        arrived(precv.at[k], pr.at[k])
        acc = [jnp.broadcast_to(bias[l:l + 1, q * block:(q + 1) * block], (size, block)) for q in range(width)]
        acc = [acc[q] + precv[k, q].astype(f32) for q in range(width)]
        for n in range(near):
            t = trecv[k, n].astype(f32)
            where = col[l, 0, source(n)]
            for q in range(width):
                acc[q] = acc[q] + t * (where == q).astype(f32)
        for q in range(width):
            act[q, c * size:(c + 1) * size, :] = jnp.maximum(acc[q], 0.0).astype(bf16)

    def split(c):
        p = c // hz
        return p, (1 - p) * (c % hz) + p * (hz - 1 - c % hz)

    def owners(c):
        p, d = split(c)
        far = (1 - hi) * (hz + d) + hi * (hz - 1 - d)
        close = hi * (hz + d) + (1 - hi) * (hz - 1 - d)
        return [(2 * j + p, far, 2 * j + 1 - hi) for j in range(nx // 2)], [(2 * j + p, close, 2 * j + hi) for j in range(nx // 2)]

    def send_last(c):
        l = layers - 1
        p, q = split(c)
        far, close = owners(c)
        for e in range(nd):
            t = product(l, c, e).reshape(per, rows, block)
            lsend[c * per:(c + 1) * per, e] = t.astype(bf16)
        for g in range(GROUPS):
            for a, b, o in far:
                send_far(c, g, q, a, o)
        release(DEPTH_LAST - 1)
        held.append([functools.partial(send_close, c, a, b, o) for a, b, o in close])

    def send_far(c, g, q, a, o):
        src, dst = lsend.at[c * per + o, g * part:(g + 1) * part], qrecv.at[q, g, slot]
        mine = jnp.logical_and(relay, my_x == a)

        @pl.when(mine)
        def _():
            pltpu.make_async_copy(src, dst, qr.at[q, g]).start()

        @pl.when(jnp.logical_not(mine))
        def _():
            remote(src, dst, ls, qr.at[q, g], a, relay_z).start()

    def send_close(c, a, b, o):
        src, dst = lsend.at[c * per + o], orecv.at[slot]
        mine = jnp.logical_and(my_z == b, my_x == a)

        @pl.when(mine)
        def _():
            pltpu.make_async_copy(src, dst, orr).start()

        @pl.when(jnp.logical_not(mine))
        def _():
            remote(src, dst, ls, orr, a, b).start()

    def forward_last(c):
        p, q = split(c)

        @pl.when(jnp.logical_and(relay, my_x % 2 == p))
        def _():
            for g in range(GROUPS):
                arrived(qrecv.at[q, g], qr.at[q, g])
                for e in range(part):
                    acc = [jnp.zeros((rows, block), f32) for r in range(width)]
                    for n in range(near):
                        t = qrecv[q, g, n, e].astype(f32)
                        v = jnp.broadcast_to(colx[pl.ds((g * part + e) * nd + source(n), 1), :], (rows, block))
                        for r in range(width):
                            acc[r] = acc[r] + jnp.where(v == float(r), t, 0.0)
                    for r in range(width):
                        usend[q, g * part + e, r] = acc[r].astype(bf16)
                piece = pl.ds(g * part, part)
                remote(usend.at[q, piece], urecv.at[piece], us, ur.at[g], my_x, (1 - hi) * (hz + q) + hi * (hz - 1 - q)).start()

    for c in range(chunks):
        arrived(fin.at[c * per:(c + 1) * per], fr.at[c])
        for r in range(width):
            x = fin[c * per:(c + 1) * per, :, r * block:(r + 1) * block].astype(f32).reshape(size, block)
            act[r, c * size:(c + 1) * size, :] = x.astype(bf16)
        if c == 0:
            arrived(w.at[0], wsem.at[0])
        send_terms(0, c)

    arrived(aux, xr)
    eye = lax.broadcasted_iota(jnp.int32, (nd, block), 0) == lax.broadcasted_iota(jnp.int32, (nd, block), 1)
    ones = jnp.ones((block, block), bf16)
    for l in range(layers - 1):
        for i in range(hz):
            v = jnp.where(eye, aux[my_x * ny + far_z + i, width + l:width + l + 1, :], 0.0).astype(bf16)
            m = jnp.dot(v, ones, preferred_element_type=f32)
            k = (l * hz + i) * nd
            colr[k:k + nd] = jnp.broadcast_to(m[:, None, :], (nd, 8, block))
    for e in range(nd):
        last = width + layers - 1
        v = jnp.where(eye, aux[e, last:last + 1, :], 0.0).astype(bf16)
        colx[e * nd:(e + 1) * nd, :] = jnp.dot(v, ones, preferred_element_type=f32)

    total = layers * chunks

    def relay_step(k):
        if k < total - chunks:
            forward(k // chunks, k % chunks)
        elif k < total:
            forward_last(k % chunks)

    for k in range(LAG):
        relay_step(k)
    for k in range(total - chunks):
        relay_step(k + LAG)
        l, c = k // chunks, k % chunks
        collect(l, c)
        if c == 0:
            arrived(w.at[l + 1], wsem.at[l + 1])
        if l + 1 < layers - 1:
            send_terms(l + 1, c)
        else:
            send_last(c)
    release(0)
    for k in range(total - chunks + LAG, total):
        relay_step(k)

    arrived(orecv, orr)
    for e in range(nd):
        acc = [jnp.broadcast_to(aux[e, q:q + 1, :], (rows, block)) for q in range(width)]
        for n in range(near):
            t = orecv[n, e].astype(f32)
            v = jnp.broadcast_to(colx[pl.ds(e * nd + source(n), 1), :], (rows, block))
            for q in range(width):
                acc[q] = acc[q] + jnp.where(v == float(q), t, 0.0)
        for q in range(width):
            pre[e * width + q] = acc[q]
    for g in range(GROUPS):
        piece = urecv.at[g * part:(g + 1) * part]
        arrived(piece, ur.at[g])
        for e in range(g * part, (g + 1) * part):
            for q in range(width):
                s = (e * width + q) * block
                out[:, s:s + block] = jnp.maximum(pre[e * width + q] + urecv[e, q].astype(f32), 0.0).astype(bf16)

    arrived(fin.at[0:nd - 1], fs)
    arrived(aux.at[0:nd - 1], xs)
    arrived(tsend.at[0:near - 1], ts)
    arrived(rsend.at[0:nx - 1], rs)

    @pl.when(relay)
    def _():
        arrived(psend, ps)
        arrived(usend, us)
        arrived(lsend.at[0:nd - 1 - hz], ls)

    @pl.when(jnp.logical_not(relay))
    def _():
        arrived(rsend.at[nx - 1], ro)
        arrived(lsend.at[0:nd - 1], ls)


def fused(nx, ny, features, link_weight, link_row, link_col, link_live, bias):
    nd = nx * ny
    layers = bias.shape[0]
    block = link_weight.shape[-1]
    width = bias.shape[1] // block
    rows = features.shape[0]
    hz = ny // 2
    chunks = 2 * hz
    per = nd // chunks
    size = per * rows
    near = nx * hz
    steps = (layers - 1) * chunks
    bf16, f32 = jnp.bfloat16, jnp.float32
    vmem = pltpu.VMEM
    counts = pltpu.SMEM((layers, 1, nd), jnp.int32)
    dma = pltpu.SemaphoreType.DMA
    return pl.pallas_call(
        functools.partial(kernel, nx, ny),
        out_shape=vmem(features.shape, bf16),
        in_specs=[pl.BlockSpec(memory_space=pl.ANY)] * 6,
        out_specs=pl.BlockSpec(memory_space=vmem),
        scratch_shapes=[
            vmem(features.shape, bf16), counts, counts, counts, vmem(bias.shape, f32), dma((5,)),
            vmem((layers, nd, block, block), bf16), dma((layers,)),
            vmem((nd, rows, width * block), bf16), dma, dma((chunks,)),
            vmem((width, rows * nd, block), bf16),
            vmem((8, block), f32), vmem((nd, 8, block), f32), dma, dma,
            vmem((nd * nd, block), f32), vmem(((layers - 1) * hz * nd, 8, block), f32),
            vmem((near, steps, size, block), bf16), vmem((steps, near, size, block), bf16), dma, dma((steps,)),
            vmem((nx, steps, hz, size, block), bf16), vmem((steps, near, hz, size, block), bf16), dma, dma, dma((steps,)),
            vmem((steps, hz, width, size, block), bf16), vmem((steps, width, size, block), bf16), dma, dma((steps,)),
            vmem((nd, nd, rows, block), bf16), vmem((near, nd, rows, block), bf16), dma, dma,
            vmem((hz, GROUPS, near, nd // GROUPS, rows, block), bf16), dma((hz, GROUPS)),
            vmem((hz, nd, width, rows, block), bf16), vmem((nd, width, rows, block), bf16), dma, dma((GROUPS,)),
            vmem((nd * width, rows, block), f32),
        ],
        compiler_params=pltpu.CompilerParams(
            collective_id=0, has_side_effects=True, vmem_limit_bytes=60 * 1024 * 1024
        ),
    )(features, link_weight, link_row, jnp.transpose(link_col, (0, 2, 1)), link_live, bias)


def solution(mesh):
    placed = (
        P(("nx", "ny", "img"), None),
        P(None, ("nx", "ny"), None, None, None),
        P(None, ("nx", "ny"), None),
        P(None, None, ("nx", "ny")),
        P(None, ("nx", "ny"), None),
        P(None, ("nx", "ny")),
    )
    nx, ny = mesh.shape["nx"], mesh.shape["ny"]

    def run(features, link_weight, link_row, link_col, link_live, bias):
        block = link_weight.shape[-1]
        rows = features.shape[0]
        width = bias.shape[1] // block
        fits = (
            rows % 8 == 0 and nx % 2 == 0 and ny % 2 == 0 and block == 128
            and nx * ny <= 32 and nx * ny % GROUPS == 0 and width + bias.shape[0] <= 8 and (nx * rows) % 16 == 0 and bias.shape[0] > 1
        )
        step = functools.partial(fused, nx, ny) if fits else local
        return step(features, link_weight, link_row, link_col, link_live, bias)

    return jax.shard_map(
        run, mesh=mesh, in_specs=placed, out_specs=P(("nx", "ny", "img"), None), check_vma=False
    )
```

```python
import functools

import jax
import jax.numpy as jnp
from jax import lax
from jax.experimental import pallas as pl
from jax.experimental.pallas import tpu as pltpu
from jax.sharding import PartitionSpec as P

MESH = pl.DeviceIdType.MESH
LAG = 1
GROUPS = 4
DEPTH = 1
DEPTH_LAST = 1


def combine_links(received, col_ids, width):
    onehot = (col_ids[:, None] == jnp.arange(width, dtype=jnp.int32)[None, :]).astype(jnp.bfloat16)
    summed = jnp.einsum("dq,dis->iqs", onehot, received, preferred_element_type=jnp.float32)
    return summed.reshape(summed.shape[0], width * received.shape[2])


def link_products(blocks, weights, row_ids, live_mask):
    masked = weights * live_mask.astype(jnp.bfloat16)[:, None, None]
    gathered = jnp.take(blocks, row_ids, axis=1)
    result = jnp.einsum(
        "ier,ers->eis", gathered, masked, preferred_element_type=jnp.float32
    ).astype(jnp.bfloat16)
    return result


def local(features, link_weight, link_row, link_col, link_live, bias):
    block_size = link_weight.shape[-1]
    width = bias.shape[1] // block_size
    hidden = lax.all_to_all(features, ("nx", "ny"), split_axis=1, concat_axis=0, tiled=True)
    image_rows = hidden.shape[0]
    for layer_idx in range(bias.shape[0]):
        blocks = hidden.reshape(image_rows, width, block_size)
        link_terms = link_products(
            blocks, link_weight[layer_idx, 0], link_row[layer_idx, 0], link_live[layer_idx, 0]
        )
        col_ids = link_col[layer_idx, :, 0]
        summed = combine_links(
            lax.all_to_all(link_terms, ("nx", "ny"), split_axis=0, concat_axis=0, tiled=True),
            col_ids,
            width,
        )
        hidden = jnp.maximum(summed + bias[layer_idx][None, :], 0.0).astype(jnp.bfloat16)
    finished = lax.all_to_all(hidden, ("nx", "ny"), split_axis=0, concat_axis=1, tiled=True)
    return finished


def kernel(nx, ny, feat_hbm, weight_hbm, row_hbm, col_hbm, live_hbm, bias_hbm, out, feat, row, col, live, bias, isem, w, wsem,
           fin, fs, fr, act, auxs, aux, xs, xr, colx, colr, tsend, trecv, ts, tr, rsend, rrecv, rs, ro, rr, psend, precv, ps, pr,
           lsend, orecv, ls, orr, qrecv, qr, usend, urecv, us, ur, pre):
    nd = nx * ny
    layers = bias.shape[0]
    block = w.shape[-1]
    width = bias.shape[1] // block
    rows = feat.shape[0]
    hz = ny // 2
    chunks = 2 * hz
    per = nd // chunks
    size = per * rows
    near = nx * hz
    f32, bf16 = jnp.float32, jnp.bfloat16
    part = nd // GROUPS
    my_x, my_z = lax.axis_index("nx"), lax.axis_index("ny")
    me = my_x * ny + my_z
    hi, lo = my_z // hz, my_z % hz
    far_z, relay_z = (1 - hi) * hz, hi + hz - 1
    relay = my_z == relay_z
    slot = my_x * hz + lo

    zs = [hi * i + (1 - hi) * (ny - 1 - i) for i in range(hz)] + [hi * hz + (lo + i) % hz for i in range(1, hz)] + [my_z]
    peers = [((my_x + i) % nx, z, i == 0 and n == ny - 1) for n, z in enumerate(zs) for i in list(range(1, nx)) + [0]]

    def place(a, b):
        d = (b // hz) * (b - hz) + (1 - b // hz) * (hz - 1 - b)
        p = a % 2
        return ((hz - 1 - d) * 2 + p) * per + (a // 2) * 2 + b // hz

    def remote(src, dst, send_sem, recv_sem, a, b):
        return pltpu.make_async_remote_copy(src, dst, send_sem, recv_sem, device_id={"nx": a, "ny": b}, device_id_type=MESH)

    def send(src, dst, send_sem, recv_sem, a, b, own):
        if own:
            pltpu.make_async_copy(src, dst, recv_sem).start()
        else:
            remote(src, dst, send_sem, recv_sem, a, b).start()

    def arrived(ref, sem):
        pltpu.make_async_copy(ref, ref, sem).wait()

    loads = [
        pltpu.make_async_copy(src, dst, isem.at[n])
        for n, (src, dst) in enumerate(((feat_hbm, feat), (bias_hbm, bias), (col_hbm, col), (row_hbm, row), (live_hbm, live)))
    ]
    for load in loads:
        load.start()
    for l in range(layers):
        pltpu.make_async_copy(weight_hbm.at[l, 0], w.at[l], wsem.at[l]).start()
    barrier = pltpu.get_barrier_semaphore()
    for a, b, own in peers:
        if not own:
            pl.semaphore_signal(barrier, inc=1, device_id={"nx": a, "ny": b}, device_id_type=MESH)

    for load in loads:
        load.wait()
    lane = lax.broadcasted_iota(jnp.int32, (1, block), 1)
    auxs[...] = jnp.zeros_like(auxs)
    for r in range(width):
        auxs[r:r + 1, :] = bias[layers - 1:layers, r * block:(r + 1) * block]
    for l in range(layers):
        cols = jnp.zeros((1, block), jnp.int32)
        for s in range(nd):
            cols = jnp.where(lane == s, col[l, 0, s], cols)
        auxs[width + l:width + l + 1, :] = cols.astype(f32)
    pl.semaphore_wait(barrier, nd - 1)

    my_place = place(my_x, my_z)
    my_chunk = my_place // per
    span = width * block
    for a, b, own in peers:
        at = pl.multiple_of((a * ny + b) * span, span)
        send(feat.at[:, pl.ds(at, span)], fin.at[my_place], fs, fr.at[my_chunk], a, b, own)
    for a, b, own in peers:
        send(auxs, aux.at[me], xs, xr, a, b, own)

    def product(l, c, e):
        x = act[row[l, 0, e], c * size:(c + 1) * size, :]
        t = jnp.dot(x, w[l, e], preferred_element_type=f32)
        return t * live[l, 0, e].astype(f32)

    def source(n):
        return (n // hz) * ny + hi * hz + n % hz

    order = list(range(1, nx)) + [0]
    steps = [(n, i) for n in list(range(1, hz)) + [0] for i in order]

    held = []

    def release(depth):
        while len(held) > depth:
            for start in held.pop(0):
                start()

    def send_bundle(l, c, j, i):
        k = l * chunks + c
        a = (my_x + i) % nx
        src, dst = rsend.at[j, k], rrecv.at[k, slot]
        if i == 0:
            @pl.when(relay)
            def _():
                pltpu.make_async_copy(src, dst, rr.at[k]).start()

            @pl.when(jnp.logical_not(relay))
            def _():
                remote(src, dst, ro, rr.at[k], a, relay_z).start()
        else:
            remote(src, dst, rs, rr.at[k], a, relay_z).start()

    def send_near(k, j, n, i):
        a, b = (my_x + i) % nx, hi * hz + (lo + n) % hz
        send(tsend.at[j, k], trecv.at[k, slot], ts, tr.at[k], a, b, n == 0 and i == 0)

    def send_terms(l, c):
        k = l * chunks + c
        for j, i in enumerate(order):
            for n in range(hz):
                rsend[j, k, n] = product(l, c, (my_x + i) % nx * ny + far_z + n).astype(bf16)
        for j, i in enumerate(order):
            send_bundle(l, c, j, i)
        release(DEPTH - 1)
        for j, (n, i) in enumerate(steps):
            tsend[j, k] = product(l, c, (my_x + i) % nx * ny + hi * hz + (lo + n) % hz).astype(bf16)
        held.append([functools.partial(send_near, k, j, n, i) for j, (n, i) in enumerate(steps)])

    def forward(l, c):
        k = l * chunks + c

        @pl.when(relay)
        def _():
            arrived(rrecv.at[k], rr.at[k])
            for i in range(hz):
                acc = [jnp.zeros((size, block), f32) for q in range(width)]
                for n in range(near):
                    t = rrecv[k, n, i].astype(f32)
                    v = colr[pl.ds((l * hz + i) * nd + source(n), 1)][0]
                    v = jnp.concatenate([v] * (size // 8), axis=0)
                    for q in range(width):
                        acc[q] = acc[q] + jnp.where(v == float(q), t, 0.0)
                for q in range(width):
                    psend[k, i, q] = acc[q].astype(bf16)
                remote(psend.at[k, i], precv.at[k], ps, pr.at[k], my_x, far_z + i).start()

    def collect(l, c):
        k = l * chunks + c
        arrived(trecv.at[k], tr.at[k])
        arrived(precv.at[k], pr.at[k])
        acc = [jnp.broadcast_to(bias[l:l + 1, q * block:(q + 1) * block], (size, block)) for q in range(width)]
        acc = [acc[q] + precv[k, q].astype(f32) for q in range(width)]
        for n in range(near):
            t = trecv[k, n].astype(f32)
            where = col[l, 0, source(n)]
            for q in range(width):
                acc[q] = acc[q] + t * (where == q).astype(f32)
        for q in range(width):
            act[q, c * size:(c + 1) * size, :] = jnp.maximum(acc[q], 0.0).astype(bf16)

    def split(c):
        return c % 2, hz - 1 - c // 2

    def owners(c):
        p, d = split(c)
        far = (1 - hi) * (hz + d) + hi * (hz - 1 - d)
        close = hi * (hz + d) + (1 - hi) * (hz - 1 - d)
        return [(2 * j + p, far, 2 * j + 1 - hi) for j in range(nx // 2)], [(2 * j + p, close, 2 * j + hi) for j in range(nx // 2)]

    def send_last(c):
        l = layers - 1
        p, q = split(c)
        far, close = owners(c)
        for e in range(nd):
            t = product(l, c, e).reshape(per, rows, block)
            lsend[c * per:(c + 1) * per, e] = t.astype(bf16)
        for g in range(GROUPS):
            for a, b, o in far:
                send_far(c, g, q, a, o)
        release(DEPTH_LAST - 1)
        held.append([functools.partial(send_close, c, a, b, o) for a, b, o in close])

    def send_far(c, g, q, a, o):
        src, dst = lsend.at[c * per + o, g * part:(g + 1) * part], qrecv.at[q, g, slot]
        mine = jnp.logical_and(relay, my_x == a)

        @pl.when(mine)
        def _():
            pltpu.make_async_copy(src, dst, qr.at[q, g]).start()

        @pl.when(jnp.logical_not(mine))
        def _():
            remote(src, dst, ls, qr.at[q, g], a, relay_z).start()

    def send_close(c, a, b, o):
        src, dst = lsend.at[c * per + o], orecv.at[slot]
        mine = jnp.logical_and(my_z == b, my_x == a)

        @pl.when(mine)
        def _():
            pltpu.make_async_copy(src, dst, orr).start()

        @pl.when(jnp.logical_not(mine))
        def _():
            remote(src, dst, ls, orr, a, b).start()

    def forward_last(c):
        p, q = split(c)

        @pl.when(jnp.logical_and(relay, my_x % 2 == p))
        def _():
            for g in range(GROUPS):
                arrived(qrecv.at[q, g], qr.at[q, g])
                for e in range(part):
                    acc = [jnp.zeros((rows, block), f32) for r in range(width)]
                    for n in range(near):
                        t = qrecv[q, g, n, e].astype(f32)
                        v = jnp.broadcast_to(colx[pl.ds((g * part + e) * nd + source(n), 1), :], (rows, block))
                        for r in range(width):
                            acc[r] = acc[r] + jnp.where(v == float(r), t, 0.0)
                    for r in range(width):
                        usend[q, g * part + e, r] = acc[r].astype(bf16)
                piece = pl.ds(g * part, part)
                remote(usend.at[q, piece], urecv.at[piece], us, ur.at[g], my_x, (1 - hi) * (hz + q) + hi * (hz - 1 - q)).start()

    for c in range(chunks):
        arrived(fin.at[c * per:(c + 1) * per], fr.at[c])
        for r in range(width):
            x = fin[c * per:(c + 1) * per, :, r * block:(r + 1) * block].astype(f32).reshape(size, block)
            act[r, c * size:(c + 1) * size, :] = x.astype(bf16)
        if c == 0:
            arrived(w.at[0], wsem.at[0])
        send_terms(0, c)

    arrived(aux, xr)
    eye = lax.broadcasted_iota(jnp.int32, (nd, block), 0) == lax.broadcasted_iota(jnp.int32, (nd, block), 1)
    ones = jnp.ones((block, block), bf16)
    for l in range(layers - 1):
        for i in range(hz):
            v = jnp.where(eye, aux[my_x * ny + far_z + i, width + l:width + l + 1, :], 0.0).astype(bf16)
            m = jnp.dot(v, ones, preferred_element_type=f32)
            k = (l * hz + i) * nd
            colr[k:k + nd] = jnp.broadcast_to(m[:, None, :], (nd, 8, block))
    for e in range(nd):
        last = width + layers - 1
        v = jnp.where(eye, aux[e, last:last + 1, :], 0.0).astype(bf16)
        colx[e * nd:(e + 1) * nd, :] = jnp.dot(v, ones, preferred_element_type=f32)

    total = layers * chunks

    def relay_step(k):
        if k < total - chunks:
            forward(k // chunks, k % chunks)
        elif k < total:
            forward_last(k % chunks)

    for k in range(LAG):
        relay_step(k)
    for k in range(total - chunks):
        relay_step(k + LAG)
        l, c = k // chunks, k % chunks
        collect(l, c)
        if c == 0:
            arrived(w.at[l + 1], wsem.at[l + 1])
        if l + 1 < layers - 1:
            send_terms(l + 1, c)
        else:
            send_last(c)
    release(0)
    for k in range(total - chunks + LAG, total):
        relay_step(k)

    arrived(orecv, orr)
    for e in range(nd):
        acc = [jnp.broadcast_to(aux[e, q:q + 1, :], (rows, block)) for q in range(width)]
        for n in range(near):
            t = orecv[n, e].astype(f32)
            v = jnp.broadcast_to(colx[pl.ds(e * nd + source(n), 1), :], (rows, block))
            for q in range(width):
                acc[q] = acc[q] + jnp.where(v == float(q), t, 0.0)
        for q in range(width):
            pre[e * width + q] = acc[q]
    for g in range(GROUPS):
        piece = urecv.at[g * part:(g + 1) * part]
        arrived(piece, ur.at[g])
        for e in range(g * part, (g + 1) * part):
            for q in range(width):
                s = (e * width + q) * block
                out[:, s:s + block] = jnp.maximum(pre[e * width + q] + urecv[e, q].astype(f32), 0.0).astype(bf16)

    arrived(fin.at[0:nd - 1], fs)
    arrived(aux.at[0:nd - 1], xs)
    arrived(tsend.at[0:near - 1], ts)
    arrived(rsend.at[0:nx - 1], rs)

    @pl.when(relay)
    def _():
        arrived(psend, ps)
        arrived(usend, us)
        arrived(lsend.at[0:nd - 1 - hz], ls)

    @pl.when(jnp.logical_not(relay))
    def _():
        arrived(rsend.at[nx - 1], ro)
        arrived(lsend.at[0:nd - 1], ls)


def fused(nx, ny, features, link_weight, link_row, link_col, link_live, bias):
    nd = nx * ny
    layers = bias.shape[0]
    block = link_weight.shape[-1]
    width = bias.shape[1] // block
    rows = features.shape[0]
    hz = ny // 2
    chunks = 2 * hz
    per = nd // chunks
    size = per * rows
    near = nx * hz
    steps = (layers - 1) * chunks
    bf16, f32 = jnp.bfloat16, jnp.float32
    vmem = pltpu.VMEM
    counts = pltpu.SMEM((layers, 1, nd), jnp.int32)
    dma = pltpu.SemaphoreType.DMA
    return pl.pallas_call(
        functools.partial(kernel, nx, ny),
        out_shape=vmem(features.shape, bf16),
        in_specs=[pl.BlockSpec(memory_space=pl.ANY)] * 6,
        out_specs=pl.BlockSpec(memory_space=vmem),
        scratch_shapes=[
            vmem(features.shape, bf16), counts, counts, counts, vmem(bias.shape, f32), dma((5,)),
            vmem((layers, nd, block, block), bf16), dma((layers,)),
            vmem((nd, rows, width * block), bf16), dma, dma((chunks,)),
            vmem((width, rows * nd, block), bf16),
            vmem((8, block), f32), vmem((nd, 8, block), f32), dma, dma,
            vmem((nd * nd, block), f32), vmem(((layers - 1) * hz * nd, 8, block), f32),
            vmem((near, steps, size, block), bf16), vmem((steps, near, size, block), bf16), dma, dma((steps,)),
            vmem((nx, steps, hz, size, block), bf16), vmem((steps, near, hz, size, block), bf16), dma, dma, dma((steps,)),
            vmem((steps, hz, width, size, block), bf16), vmem((steps, width, size, block), bf16), dma, dma((steps,)),
            vmem((nd, nd, rows, block), bf16), vmem((near, nd, rows, block), bf16), dma, dma,
            vmem((hz, GROUPS, near, nd // GROUPS, rows, block), bf16), dma((hz, GROUPS)),
            vmem((hz, nd, width, rows, block), bf16), vmem((nd, width, rows, block), bf16), dma, dma((GROUPS,)),
            vmem((nd * width, rows, block), f32),
        ],
        compiler_params=pltpu.CompilerParams(
            collective_id=0, has_side_effects=True, vmem_limit_bytes=60 * 1024 * 1024
        ),
    )(features, link_weight, link_row, jnp.transpose(link_col, (0, 2, 1)), link_live, bias)


def solution(mesh):
    placed = (
        P(("nx", "ny", "img"), None),
        P(None, ("nx", "ny"), None, None, None),
        P(None, ("nx", "ny"), None),
        P(None, None, ("nx", "ny")),
        P(None, ("nx", "ny"), None),
        P(None, ("nx", "ny")),
    )
    nx, ny = mesh.shape["nx"], mesh.shape["ny"]

    def run(features, link_weight, link_row, link_col, link_live, bias):
        block = link_weight.shape[-1]
        rows = features.shape[0]
        width = bias.shape[1] // block
        fits = (
            rows % 8 == 0 and nx % 2 == 0 and ny % 2 == 0 and block == 128
            and nx * ny <= 32 and nx * ny % GROUPS == 0 and width + bias.shape[0] <= 8 and (nx * rows) % 16 == 0 and bias.shape[0] > 1
        )
        step = functools.partial(fused, nx, ny) if fits else local
        return step(features, link_weight, link_row, link_col, link_live, bias)

    return jax.shard_map(
        run, mesh=mesh, in_specs=placed, out_specs=P(("nx", "ny", "img"), None), check_vma=False
    )
```

```python
import functools

import jax
import jax.numpy as jnp
from jax import lax
from jax.experimental import pallas as pl
from jax.experimental.pallas import tpu as pltpu
from jax.sharding import PartitionSpec as P

MESH = pl.DeviceIdType.MESH
LAG = 1
GROUPS = 4
DEPTH = 1
DEPTH_LAST = 1


def combine_links(received, col_ids, width):
    onehot = (col_ids[:, None] == jnp.arange(width, dtype=jnp.int32)[None, :]).astype(jnp.bfloat16)
    summed = jnp.einsum("dq,dis->iqs", onehot, received, preferred_element_type=jnp.float32)
    return summed.reshape(summed.shape[0], width * received.shape[2])


def link_products(blocks, weights, row_ids, live_mask):
    masked = weights * live_mask.astype(jnp.bfloat16)[:, None, None]
    gathered = jnp.take(blocks, row_ids, axis=1)
    result = jnp.einsum(
        "ier,ers->eis", gathered, masked, preferred_element_type=jnp.float32
    ).astype(jnp.bfloat16)
    return result


def local(features, link_weight, link_row, link_col, link_live, bias):
    block_size = link_weight.shape[-1]
    width = bias.shape[1] // block_size
    hidden = lax.all_to_all(features, ("nx", "ny"), split_axis=1, concat_axis=0, tiled=True)
    image_rows = hidden.shape[0]
    for layer_idx in range(bias.shape[0]):
        blocks = hidden.reshape(image_rows, width, block_size)
        link_terms = link_products(
            blocks, link_weight[layer_idx, 0], link_row[layer_idx, 0], link_live[layer_idx, 0]
        )
        col_ids = link_col[layer_idx, :, 0]
        summed = combine_links(
            lax.all_to_all(link_terms, ("nx", "ny"), split_axis=0, concat_axis=0, tiled=True),
            col_ids,
            width,
        )
        hidden = jnp.maximum(summed + bias[layer_idx][None, :], 0.0).astype(jnp.bfloat16)
    finished = lax.all_to_all(hidden, ("nx", "ny"), split_axis=0, concat_axis=1, tiled=True)
    return finished


def kernel(nx, ny, feat_hbm, weight_hbm, row_hbm, col_hbm, live_hbm, bias_hbm, out, feat, row, col, live, bias, isem, w, wsem,
           fin, fs, fr, act, cols, bias_out, colg, cs, cr, pair, ns, nr, biasg, bs, br, colx, colr, tsend, trecv, ts, tr, rsend, rrecv, rs, ro, rr, psend, precv, ps, pr,
           lsend, orecv, ls, orr, qrecv, qr, usend, urecv, us, ur, pre):
    nd = nx * ny
    layers = bias.shape[0]
    block = w.shape[-1]
    width = bias.shape[1] // block
    rows = feat.shape[0]
    hz = ny // 2
    chunks = 2 * hz
    per = nd // chunks
    size = per * rows
    near = nx * hz
    f32, bf16 = jnp.float32, jnp.bfloat16
    part = nd // GROUPS
    my_x, my_z = lax.axis_index("nx"), lax.axis_index("ny")
    me = my_x * ny + my_z
    hi, lo = my_z // hz, my_z % hz
    far_z, relay_z = (1 - hi) * hz, hi + hz - 1
    relay = my_z == relay_z
    slot = my_x * hz + lo

    zs = [hi * i + (1 - hi) * (ny - 1 - i) for i in range(hz)] + [hi * hz + (lo + i) % hz for i in range(1, hz)] + [my_z]
    peers = [((my_x + i) % nx, z, i == 0 and n == ny - 1) for n, z in enumerate(zs) for i in list(range(1, nx)) + [0]]

    def place(a, b):
        d = (b // hz) * (b - hz) + (1 - b // hz) * (hz - 1 - b)
        p = a % 2
        return ((hz - 1 - d) * 2 + p) * per + (a // 2) * 2 + b // hz

    def remote(src, dst, send_sem, recv_sem, a, b):
        return pltpu.make_async_remote_copy(src, dst, send_sem, recv_sem, device_id={"nx": a, "ny": b}, device_id_type=MESH)

    def send(src, dst, send_sem, recv_sem, a, b, own):
        if own:
            pltpu.make_async_copy(src, dst, recv_sem).start()
        else:
            remote(src, dst, send_sem, recv_sem, a, b).start()

    def arrived(ref, sem):
        pltpu.make_async_copy(ref, ref, sem).wait()

    loads = [
        pltpu.make_async_copy(src, dst, isem.at[n])
        for n, (src, dst) in enumerate(((feat_hbm, feat), (bias_hbm, bias), (col_hbm, col), (row_hbm, row), (live_hbm, live)))
    ]
    for load in loads:
        load.start()
    for l in range(layers):
        pltpu.make_async_copy(weight_hbm.at[l, 0], w.at[l], wsem.at[l]).start()
    barrier = pltpu.get_barrier_semaphore()
    for a, b, own in peers:
        if not own:
            pl.semaphore_signal(barrier, inc=1, device_id={"nx": a, "ny": b}, device_id_type=MESH)

    for load in loads:
        load.wait()
    lane = lax.broadcasted_iota(jnp.int32, (1, block), 1)
    cols[...] = jnp.zeros_like(cols)
    for r in range(width):
        bias_out[r:r + 1, :] = bias[layers - 1:layers, r * block:(r + 1) * block]
    for l in range(layers):
        v = jnp.zeros((1, block), jnp.int32)
        for s in range(nd):
            v = jnp.where(lane == s, col[l, 0, s], v)
        cols[l:l + 1, :] = v.astype(f32)
    pl.semaphore_wait(barrier, nd - 1)

    my_place = place(my_x, my_z)
    my_chunk = my_place // per
    span = width * block
    for a, b, own in peers:
        at = pl.multiple_of((a * ny + b) * span, span)
        send(feat.at[:, pl.ds(at, span)], fin.at[my_place], fs, fr.at[my_chunk], a, b, own)
    remote(cols, pair.at[lo], ns, nr, my_x, (1 - hi) * hz + hi * (hz - 1)).start()
    for a, b, own in peers:
        send(cols.at[layers - 1:layers], colg.at[pl.ds(me, 1)], cs, cr, a, b, own)
    for a, b, own in peers:
        send(bias_out, biasg.at[me], bs, br, a, b, own)

    def product(l, c, e):
        x = act[row[l, 0, e], c * size:(c + 1) * size, :]
        t = jnp.dot(x, w[l, e], preferred_element_type=f32)
        return t * live[l, 0, e].astype(f32)

    def source(n):
        return (n // hz) * ny + hi * hz + n % hz

    order = list(range(1, nx)) + [0]
    steps = [(n, i) for n in list(range(1, hz)) + [0] for i in order]

    held = []

    def release(depth):
        while len(held) > depth:
            for start in held.pop(0):
                start()

    def send_bundle(l, c, j, i):
        k = l * chunks + c
        a = (my_x + i) % nx
        src, dst = rsend.at[j, k], rrecv.at[k, slot]
        if i == 0:
            @pl.when(relay)
            def _():
                pltpu.make_async_copy(src, dst, rr.at[k]).start()

            @pl.when(jnp.logical_not(relay))
            def _():
                remote(src, dst, ro, rr.at[k], a, relay_z).start()
        else:
            remote(src, dst, rs, rr.at[k], a, relay_z).start()

    def send_near(k, j, n, i):
        a, b = (my_x + i) % nx, hi * hz + (lo + n) % hz
        send(tsend.at[j, k], trecv.at[k, slot], ts, tr.at[k], a, b, n == 0 and i == 0)

    def send_terms(l, c):
        k = l * chunks + c
        for j, i in enumerate(order):
            for n in range(hz):
                rsend[j, k, n] = product(l, c, (my_x + i) % nx * ny + far_z + n).astype(bf16)
        for j, i in enumerate(order):
            send_bundle(l, c, j, i)
        release(DEPTH - 1)
        for j, (n, i) in enumerate(steps):
            tsend[j, k] = product(l, c, (my_x + i) % nx * ny + hi * hz + (lo + n) % hz).astype(bf16)
        held.append([functools.partial(send_near, k, j, n, i) for j, (n, i) in enumerate(steps)])

    def forward(l, c):
        k = l * chunks + c

        @pl.when(relay)
        def _():
            arrived(rrecv.at[k], rr.at[k])
            for i in range(hz):
                acc = [jnp.zeros((size, block), f32) for q in range(width)]
                for n in range(near):
                    t = rrecv[k, n, i].astype(f32)
                    v = colr[pl.ds((l * hz + i) * nd + source(n), 1)][0]
                    v = jnp.concatenate([v] * (size // 8), axis=0)
                    for q in range(width):
                        acc[q] = acc[q] + jnp.where(v == float(q), t, 0.0)
                for q in range(width):
                    psend[k, i, q] = acc[q].astype(bf16)
                remote(psend.at[k, i], precv.at[k], ps, pr.at[k], my_x, far_z + i).start()

    def collect(l, c):
        k = l * chunks + c
        arrived(trecv.at[k], tr.at[k])
        arrived(precv.at[k], pr.at[k])
        acc = [jnp.broadcast_to(bias[l:l + 1, q * block:(q + 1) * block], (size, block)) for q in range(width)]
        acc = [acc[q] + precv[k, q].astype(f32) for q in range(width)]
        for n in range(near):
            t = trecv[k, n].astype(f32)
            where = col[l, 0, source(n)]
            for q in range(width):
                acc[q] = acc[q] + t * (where == q).astype(f32)
        for q in range(width):
            act[q, c * size:(c + 1) * size, :] = jnp.maximum(acc[q], 0.0).astype(bf16)

    def split(c):
        return c % 2, hz - 1 - c // 2

    def owners(c):
        p, d = split(c)
        far = (1 - hi) * (hz + d) + hi * (hz - 1 - d)
        close = hi * (hz + d) + (1 - hi) * (hz - 1 - d)
        return [(2 * j + p, far, 2 * j + 1 - hi) for j in range(nx // 2)], [(2 * j + p, close, 2 * j + hi) for j in range(nx // 2)]

    def send_last(c):
        l = layers - 1
        p, q = split(c)
        far, close = owners(c)
        for e in range(nd):
            t = product(l, c, e).reshape(per, rows, block)
            lsend[c * per:(c + 1) * per, e] = t.astype(bf16)
        for g in range(GROUPS):
            for a, b, o in far:
                send_far(c, g, q, a, o)
        release(DEPTH_LAST - 1)
        held.append([functools.partial(send_close, c, a, b, o) for a, b, o in close])

    def send_far(c, g, q, a, o):
        src, dst = lsend.at[c * per + o, g * part:(g + 1) * part], qrecv.at[q, g, slot]
        mine = jnp.logical_and(relay, my_x == a)

        @pl.when(mine)
        def _():
            pltpu.make_async_copy(src, dst, qr.at[q, g]).start()

        @pl.when(jnp.logical_not(mine))
        def _():
            remote(src, dst, ls, qr.at[q, g], a, relay_z).start()

    def send_close(c, a, b, o):
        src, dst = lsend.at[c * per + o], orecv.at[slot]
        mine = jnp.logical_and(my_z == b, my_x == a)

        @pl.when(mine)
        def _():
            pltpu.make_async_copy(src, dst, orr).start()

        @pl.when(jnp.logical_not(mine))
        def _():
            remote(src, dst, ls, orr, a, b).start()

    def forward_last(c):
        p, q = split(c)

        @pl.when(jnp.logical_and(relay, my_x % 2 == p))
        def _():
            for g in range(GROUPS):
                arrived(qrecv.at[q, g], qr.at[q, g])
                for e in range(part):
                    acc = [jnp.zeros((rows, block), f32) for r in range(width)]
                    for n in range(near):
                        t = qrecv[q, g, n, e].astype(f32)
                        v = jnp.broadcast_to(colx[pl.ds((g * part + e) * nd + source(n), 1), :], (rows, block))
                        for r in range(width):
                            acc[r] = acc[r] + jnp.where(v == float(r), t, 0.0)
                    for r in range(width):
                        usend[q, g * part + e, r] = acc[r].astype(bf16)
                piece = pl.ds(g * part, part)
                remote(usend.at[q, piece], urecv.at[piece], us, ur.at[g], my_x, (1 - hi) * (hz + q) + hi * (hz - 1 - q)).start()

    for c in range(chunks):
        arrived(fin.at[c * per:(c + 1) * per], fr.at[c])
        for r in range(width):
            x = fin[c * per:(c + 1) * per, :, r * block:(r + 1) * block].astype(f32).reshape(size, block)
            act[r, c * size:(c + 1) * size, :] = x.astype(bf16)
        if c == 0:
            arrived(w.at[0], wsem.at[0])
        send_terms(0, c)

    eye = lax.broadcasted_iota(jnp.int32, (nd, block), 0) == lax.broadcasted_iota(jnp.int32, (nd, block), 1)
    ones = jnp.ones((block, block), bf16)

    @pl.when(relay)
    def _():
        arrived(pair, nr)
        for l in range(layers - 1):
            for i in range(hz):
                v = jnp.where(eye, pair[i, l:l + 1, :], 0.0).astype(bf16)
                m = jnp.dot(v, ones, preferred_element_type=f32)
                k = (l * hz + i) * nd
                colr[k:k + nd] = jnp.broadcast_to(m[:, None, :], (nd, 8, block))

    arrived(colg, cr)
    for e in range(nd):
        v = jnp.where(eye, colg[e:e + 1, :], 0.0).astype(bf16)
        colx[e * nd:(e + 1) * nd, :] = jnp.dot(v, ones, preferred_element_type=f32)

    total = layers * chunks

    def relay_step(k):
        if k < total - chunks:
            forward(k // chunks, k % chunks)
        elif k < total:
            forward_last(k % chunks)

    for k in range(LAG):
        relay_step(k)
    for k in range(total - chunks):
        relay_step(k + LAG)
        l, c = k // chunks, k % chunks
        collect(l, c)
        if c == 0:
            arrived(w.at[l + 1], wsem.at[l + 1])
        if l + 1 < layers - 1:
            send_terms(l + 1, c)
        else:
            send_last(c)
    release(0)
    for k in range(total - chunks + LAG, total):
        relay_step(k)

    arrived(orecv, orr)
    arrived(biasg, br)
    for e in range(nd):
        acc = [jnp.broadcast_to(biasg[e, q:q + 1, :], (rows, block)) for q in range(width)]
        for n in range(near):
            t = orecv[n, e].astype(f32)
            v = jnp.broadcast_to(colx[pl.ds(e * nd + source(n), 1), :], (rows, block))
            for q in range(width):
                acc[q] = acc[q] + jnp.where(v == float(q), t, 0.0)
        for q in range(width):
            pre[e * width + q] = acc[q]
    for g in range(GROUPS):
        piece = urecv.at[g * part:(g + 1) * part]
        arrived(piece, ur.at[g])
        for e in range(g * part, (g + 1) * part):
            for q in range(width):
                s = (e * width + q) * block
                out[:, s:s + block] = jnp.maximum(pre[e * width + q] + urecv[e, q].astype(f32), 0.0).astype(bf16)

    arrived(fin.at[0:nd - 1], fs)
    arrived(colg.at[0:nd - 1], cs)
    arrived(cols, ns)
    arrived(biasg.at[0:nd - 1], bs)
    arrived(tsend.at[0:near - 1], ts)
    arrived(rsend.at[0:nx - 1], rs)

    @pl.when(relay)
    def _():
        arrived(psend, ps)
        arrived(usend, us)
        arrived(lsend.at[0:nd - 1 - hz], ls)

    @pl.when(jnp.logical_not(relay))
    def _():
        arrived(rsend.at[nx - 1], ro)
        arrived(lsend.at[0:nd - 1], ls)


def fused(nx, ny, features, link_weight, link_row, link_col, link_live, bias):
    nd = nx * ny
    layers = bias.shape[0]
    block = link_weight.shape[-1]
    width = bias.shape[1] // block
    rows = features.shape[0]
    hz = ny // 2
    chunks = 2 * hz
    per = nd // chunks
    size = per * rows
    near = nx * hz
    steps = (layers - 1) * chunks
    bf16, f32 = jnp.bfloat16, jnp.float32
    vmem = pltpu.VMEM
    counts = pltpu.SMEM((layers, 1, nd), jnp.int32)
    dma = pltpu.SemaphoreType.DMA
    return pl.pallas_call(
        functools.partial(kernel, nx, ny),
        out_shape=vmem(features.shape, bf16),
        in_specs=[pl.BlockSpec(memory_space=pl.ANY)] * 6,
        out_specs=pl.BlockSpec(memory_space=vmem),
        scratch_shapes=[
            vmem(features.shape, bf16), counts, counts, counts, vmem(bias.shape, f32), dma((5,)),
            vmem((layers, nd, block, block), bf16), dma((layers,)),
            vmem((nd, rows, width * block), bf16), dma, dma((chunks,)),
            vmem((width, rows * nd, block), bf16),
            vmem((8, block), f32), vmem((width, block), f32), vmem((nd, block), f32), dma, dma,
            vmem((hz, 8, block), f32), dma, dma, vmem((nd, width, block), f32), dma, dma,
            vmem((nd * nd, block), f32), vmem(((layers - 1) * hz * nd, 8, block), f32),
            vmem((near, steps, size, block), bf16), vmem((steps, near, size, block), bf16), dma, dma((steps,)),
            vmem((nx, steps, hz, size, block), bf16), vmem((steps, near, hz, size, block), bf16), dma, dma, dma((steps,)),
            vmem((steps, hz, width, size, block), bf16), vmem((steps, width, size, block), bf16), dma, dma((steps,)),
            vmem((nd, nd, rows, block), bf16), vmem((near, nd, rows, block), bf16), dma, dma,
            vmem((hz, GROUPS, near, nd // GROUPS, rows, block), bf16), dma((hz, GROUPS)),
            vmem((hz, nd, width, rows, block), bf16), vmem((nd, width, rows, block), bf16), dma, dma((GROUPS,)),
            vmem((nd * width, rows, block), f32),
        ],
        compiler_params=pltpu.CompilerParams(
            collective_id=0, has_side_effects=True, vmem_limit_bytes=60 * 1024 * 1024
        ),
    )(features, link_weight, link_row, jnp.transpose(link_col, (0, 2, 1)), link_live, bias)


def solution(mesh):
    placed = (
        P(("nx", "ny", "img"), None),
        P(None, ("nx", "ny"), None, None, None),
        P(None, ("nx", "ny"), None),
        P(None, None, ("nx", "ny")),
        P(None, ("nx", "ny"), None),
        P(None, ("nx", "ny")),
    )
    nx, ny = mesh.shape["nx"], mesh.shape["ny"]

    def run(features, link_weight, link_row, link_col, link_live, bias):
        block = link_weight.shape[-1]
        rows = features.shape[0]
        width = bias.shape[1] // block
        fits = (
            rows % 8 == 0 and nx % 2 == 0 and ny % 2 == 0 and block == 128
            and nx * ny <= 32 and nx * ny % GROUPS == 0 and bias.shape[0] <= 8 and (nx * rows) % 16 == 0 and bias.shape[0] > 1
        )
        step = functools.partial(fused, nx, ny) if fits else local
        return step(features, link_weight, link_row, link_col, link_live, bias)

    return jax.shard_map(
        run, mesh=mesh, in_specs=placed, out_specs=P(("nx", "ny", "img"), None), check_vma=False
    )
```

```python
import functools

import jax
import jax.numpy as jnp
from jax import lax
from jax.experimental import pallas as pl
from jax.experimental.pallas import tpu as pltpu
from jax.sharding import PartitionSpec as P

MESH = pl.DeviceIdType.MESH
LAG = 1
GROUPS = 4
DEPTH = 1
DEPTH_LAST = 1


def combine_links(received, col_ids, width):
    onehot = (col_ids[:, None] == jnp.arange(width, dtype=jnp.int32)[None, :]).astype(jnp.bfloat16)
    summed = jnp.einsum("dq,dis->iqs", onehot, received, preferred_element_type=jnp.float32)
    return summed.reshape(summed.shape[0], width * received.shape[2])


def link_products(blocks, weights, row_ids, live_mask):
    masked = weights * live_mask.astype(jnp.bfloat16)[:, None, None]
    gathered = jnp.take(blocks, row_ids, axis=1)
    result = jnp.einsum(
        "ier,ers->eis", gathered, masked, preferred_element_type=jnp.float32
    ).astype(jnp.bfloat16)
    return result


def local(features, link_weight, link_row, link_col, link_live, bias):
    block_size = link_weight.shape[-1]
    width = bias.shape[1] // block_size
    hidden = lax.all_to_all(features, ("nx", "ny"), split_axis=1, concat_axis=0, tiled=True)
    image_rows = hidden.shape[0]
    for layer_idx in range(bias.shape[0]):
        blocks = hidden.reshape(image_rows, width, block_size)
        link_terms = link_products(
            blocks, link_weight[layer_idx, 0], link_row[layer_idx, 0], link_live[layer_idx, 0]
        )
        col_ids = link_col[layer_idx, :, 0]
        summed = combine_links(
            lax.all_to_all(link_terms, ("nx", "ny"), split_axis=0, concat_axis=0, tiled=True),
            col_ids,
            width,
        )
        hidden = jnp.maximum(summed + bias[layer_idx][None, :], 0.0).astype(jnp.bfloat16)
    finished = lax.all_to_all(hidden, ("nx", "ny"), split_axis=0, concat_axis=1, tiled=True)
    return finished


def kernel(nx, ny, feat_hbm, weight_hbm, row_hbm, col_hbm, live_hbm, bias_hbm, out, feat, row, col, live, bias, isem, w, wsem,
           fin, fs, fr, act, cols, bias_out, colg, cs, cr, pair, ns, nr, biasg, bs, br, colx, colr, tsend, trecv, ts, tr, rsend, rrecv, rs, ro, rr, psend, precv, ps, pr,
           lsend, orecv, ls, orr, qrecv, qr, usend, urecv, us, ur, pre):
    nd = nx * ny
    layers = bias.shape[0]
    block = w.shape[-1]
    width = bias.shape[1] // block
    rows = feat.shape[0]
    hz = ny // 2
    chunks = 2 * hz
    per = nd // chunks
    size = per * rows
    near = nx * hz
    f32, bf16 = jnp.float32, jnp.bfloat16
    part = nd // GROUPS
    my_x, my_z = lax.axis_index("nx"), lax.axis_index("ny")
    me = my_x * ny + my_z
    hi, lo = my_z // hz, my_z % hz
    far_z, relay_z = (1 - hi) * hz, hi + hz - 1
    relay = my_z == relay_z
    slot = my_x * hz + lo

    zs = [hi * i + (1 - hi) * (ny - 1 - i) for i in range(hz)] + [hi * hz + (lo + i) % hz for i in range(1, hz)] + [my_z]
    peers = [((my_x + i) % nx, z, i == 0 and n == ny - 1) for n, z in enumerate(zs) for i in list(range(1, nx)) + [0]]

    def place(a, b):
        d = (b // hz) * (b - hz) + (1 - b // hz) * (hz - 1 - b)
        p = a % 2
        return ((hz - 1 - d) * 2 + p) * per + (a // 2) * 2 + b // hz

    def remote(src, dst, send_sem, recv_sem, a, b):
        return pltpu.make_async_remote_copy(src, dst, send_sem, recv_sem, device_id={"nx": a, "ny": b}, device_id_type=MESH)

    def send(src, dst, send_sem, recv_sem, a, b, own):
        if own:
            pltpu.make_async_copy(src, dst, recv_sem).start()
        else:
            remote(src, dst, send_sem, recv_sem, a, b).start()

    def arrived(ref, sem):
        pltpu.make_async_copy(ref, ref, sem).wait()

    loads = [
        pltpu.make_async_copy(src, dst, isem.at[n])
        for n, (src, dst) in enumerate(((feat_hbm, feat), (bias_hbm, bias), (col_hbm, col), (row_hbm, row), (live_hbm, live)))
    ]
    for load in loads:
        load.start()
    pltpu.make_async_copy(weight_hbm.at[:, 0], w, wsem).start()
    barrier = pltpu.get_barrier_semaphore()
    for a, b, own in peers:
        if not own:
            pl.semaphore_signal(barrier, inc=1, device_id={"nx": a, "ny": b}, device_id_type=MESH)

    loads[0].wait()
    pl.semaphore_wait(barrier, nd - 1)

    my_place = place(my_x, my_z)
    my_chunk = my_place // per
    span = width * block
    for a, b, own in peers:
        at = pl.multiple_of((a * ny + b) * span, span)
        send(feat.at[:, pl.ds(at, span)], fin.at[my_place], fs, fr.at[my_chunk], a, b, own)
    for load in loads[1:]:
        load.wait()
    lane = lax.broadcasted_iota(jnp.int32, (1, block), 1)
    cols[...] = jnp.zeros_like(cols)
    for r in range(width):
        bias_out[r:r + 1, :] = bias[layers - 1:layers, r * block:(r + 1) * block]
    for l in range(layers):
        v = jnp.zeros((1, block), jnp.int32)
        for s in range(nd):
            v = jnp.where(lane == s, col[l, 0, s], v)
        cols[l:l + 1, :] = v.astype(f32)
    remote(cols, pair.at[lo], ns, nr, my_x, (1 - hi) * hz + hi * (hz - 1)).start()
    for a, b, own in peers:
        send(cols.at[layers - 1:layers], colg.at[pl.ds(me, 1)], cs, cr, a, b, own)
    for a, b, own in peers:
        send(bias_out, biasg.at[me], bs, br, a, b, own)

    def product(l, c, e):
        x = act[row[l, 0, e], c * size:(c + 1) * size, :]
        t = jnp.dot(x, w[l, e], preferred_element_type=f32)
        return t * live[l, 0, e].astype(f32)

    def source(n):
        return (n // hz) * ny + hi * hz + n % hz

    order = list(range(1, nx)) + [0]
    steps = [(n, i) for n in list(range(1, hz)) + [0] for i in order]

    held = []

    def release(depth):
        while len(held) > depth:
            for start in held.pop(0):
                start()

    def send_bundle(l, c, j, i):
        k = l * chunks + c
        a = (my_x + i) % nx
        src, dst = rsend.at[j, k], rrecv.at[k, slot]
        if i == 0:
            @pl.when(relay)
            def _():
                pltpu.make_async_copy(src, dst, rr.at[k]).start()

            @pl.when(jnp.logical_not(relay))
            def _():
                remote(src, dst, ro, rr.at[k], a, relay_z).start()
        else:
            remote(src, dst, rs, rr.at[k], a, relay_z).start()

    def send_near(k, j, n, i):
        a, b = (my_x + i) % nx, hi * hz + (lo + n) % hz
        send(tsend.at[j, k], trecv.at[k, slot], ts, tr.at[k], a, b, n == 0 and i == 0)

    def send_terms(l, c):
        k = l * chunks + c
        for j, i in enumerate(order):
            for n in range(hz):
                rsend[j, k, n] = product(l, c, (my_x + i) % nx * ny + far_z + n).astype(bf16)
        for j, i in enumerate(order):
            send_bundle(l, c, j, i)
        release(DEPTH - 1)
        for j, (n, i) in enumerate(steps):
            tsend[j, k] = product(l, c, (my_x + i) % nx * ny + hi * hz + (lo + n) % hz).astype(bf16)
        held.append([functools.partial(send_near, k, j, n, i) for j, (n, i) in enumerate(steps)])

    def forward(l, c):
        k = l * chunks + c

        @pl.when(relay)
        def _():
            arrived(rrecv.at[k], rr.at[k])
            for i in range(hz):
                z = hi * i + (1 - hi) * (hz - 1 - i)
                acc = [jnp.zeros((size, block), f32) for q in range(width)]
                for n in range(near):
                    t = rrecv[k, n, z].astype(f32)
                    v = colr[pl.ds((l * hz + z) * nd + source(n), 1)][0]
                    v = jnp.concatenate([v] * (size // 8), axis=0)
                    for q in range(width):
                        acc[q] = acc[q] + jnp.where(v == float(q), t, 0.0)
                for q in range(width):
                    psend[k, i, q] = acc[q].astype(bf16)
                remote(psend.at[k, i], precv.at[k], ps, pr.at[k], my_x, far_z + z).start()

    def collect(l, c):
        k = l * chunks + c
        arrived(trecv.at[k], tr.at[k])
        arrived(precv.at[k], pr.at[k])
        acc = [jnp.broadcast_to(bias[l:l + 1, q * block:(q + 1) * block], (size, block)) for q in range(width)]
        acc = [acc[q] + precv[k, q].astype(f32) for q in range(width)]
        for n in range(near):
            t = trecv[k, n].astype(f32)
            where = col[l, 0, source(n)]
            for q in range(width):
                acc[q] = acc[q] + t * (where == q).astype(f32)
        for q in range(width):
            act[q, c * size:(c + 1) * size, :] = jnp.maximum(acc[q], 0.0).astype(bf16)

    def split(c):
        return c % 2, hz - 1 - c // 2

    def owners(c):
        p, d = split(c)
        far = (1 - hi) * (hz + d) + hi * (hz - 1 - d)
        close = hi * (hz + d) + (1 - hi) * (hz - 1 - d)
        return [(2 * j + p, far, 2 * j + 1 - hi) for j in range(nx // 2)], [(2 * j + p, close, 2 * j + hi) for j in range(nx // 2)]

    def send_last(c):
        l = layers - 1
        p, q = split(c)
        far, close = owners(c)
        for e in range(nd):
            t = product(l, c, e).reshape(per, rows, block)
            lsend[c * per:(c + 1) * per, e] = t.astype(bf16)
        for g in range(GROUPS):
            for a, b, o in far:
                send_far(c, g, q, a, o)
        release(DEPTH_LAST - 1)
        held.append([functools.partial(send_close, c, a, b, o) for a, b, o in close])

    def send_far(c, g, q, a, o):
        src, dst = lsend.at[c * per + o, g * part:(g + 1) * part], qrecv.at[q, g, slot]
        mine = jnp.logical_and(relay, my_x == a)

        @pl.when(mine)
        def _():
            pltpu.make_async_copy(src, dst, qr.at[q, g]).start()

        @pl.when(jnp.logical_not(mine))
        def _():
            remote(src, dst, ls, qr.at[q, g], a, relay_z).start()

    def send_close(c, a, b, o):
        src, dst = lsend.at[c * per + o], orecv.at[slot]
        mine = jnp.logical_and(my_z == b, my_x == a)

        @pl.when(mine)
        def _():
            pltpu.make_async_copy(src, dst, orr).start()

        @pl.when(jnp.logical_not(mine))
        def _():
            remote(src, dst, ls, orr, a, b).start()

    def forward_last(c):
        p, q = split(c)

        @pl.when(jnp.logical_and(relay, my_x % 2 == p))
        def _():
            for g in range(GROUPS):
                arrived(qrecv.at[q, g], qr.at[q, g])
                for e in range(part):
                    acc = [jnp.zeros((rows, block), f32) for r in range(width)]
                    for n in range(near):
                        t = qrecv[q, g, n, e].astype(f32)
                        v = jnp.broadcast_to(colx[pl.ds((g * part + e) * nd + source(n), 1), :], (rows, block))
                        for r in range(width):
                            acc[r] = acc[r] + jnp.where(v == float(r), t, 0.0)
                    for r in range(width):
                        usend[q, g * part + e, r] = acc[r].astype(bf16)
                piece = pl.ds(g * part, part)
                remote(usend.at[q, piece], urecv.at[piece], us, ur.at[g], my_x, (1 - hi) * (hz + q) + hi * (hz - 1 - q)).start()

    for c in range(chunks):
        arrived(fin.at[c * per:(c + 1) * per], fr.at[c])
        for r in range(width):
            x = fin[c * per:(c + 1) * per, :, r * block:(r + 1) * block].astype(f32).reshape(size, block)
            act[r, c * size:(c + 1) * size, :] = x.astype(bf16)
        if c == 0:
            arrived(w, wsem)
        send_terms(0, c)

    eye = lax.broadcasted_iota(jnp.int32, (nd, block), 0) == lax.broadcasted_iota(jnp.int32, (nd, block), 1)
    ones = jnp.ones((block, block), bf16)

    @pl.when(relay)
    def _():
        arrived(pair, nr)
        for l in range(layers - 1):
            for i in range(hz):
                v = jnp.where(eye, pair[i, l:l + 1, :], 0.0).astype(bf16)
                m = jnp.dot(v, ones, preferred_element_type=f32)
                k = (l * hz + i) * nd
                colr[k:k + nd] = jnp.broadcast_to(m[:, None, :], (nd, 8, block))

    arrived(colg, cr)
    for e in range(nd):
        v = jnp.where(eye, colg[e:e + 1, :], 0.0).astype(bf16)
        colx[e * nd:(e + 1) * nd, :] = jnp.dot(v, ones, preferred_element_type=f32)

    total = layers * chunks

    def relay_step(k):
        if k < total - chunks:
            forward(k // chunks, k % chunks)
        elif k < total:
            forward_last(k % chunks)

    for k in range(LAG):
        relay_step(k)
    for k in range(total - chunks):
        relay_step(k + LAG)
        l, c = k // chunks, k % chunks
        collect(l, c)
        if l + 1 < layers - 1:
            send_terms(l + 1, c)
        else:
            send_last(c)
    release(0)
    for k in range(total - chunks + LAG, total):
        relay_step(k)

    arrived(orecv, orr)
    arrived(biasg, br)
    for e in range(nd):
        acc = [jnp.broadcast_to(biasg[e, q:q + 1, :], (rows, block)) for q in range(width)]
        for n in range(near):
            t = orecv[n, e].astype(f32)
            v = jnp.broadcast_to(colx[pl.ds(e * nd + source(n), 1), :], (rows, block))
            for q in range(width):
                acc[q] = acc[q] + jnp.where(v == float(q), t, 0.0)
        for q in range(width):
            pre[e * width + q] = acc[q]
    for g in range(GROUPS):
        piece = urecv.at[g * part:(g + 1) * part]
        arrived(piece, ur.at[g])
        for e in range(g * part, (g + 1) * part):
            for q in range(width):
                s = (e * width + q) * block
                out[:, s:s + block] = jnp.maximum(pre[e * width + q] + urecv[e, q].astype(f32), 0.0).astype(bf16)

    arrived(fin.at[0:nd - 1], fs)
    arrived(colg.at[0:nd - 1], cs)
    arrived(cols, ns)
    arrived(biasg.at[0:nd - 1], bs)
    arrived(tsend.at[0:near - 1], ts)
    arrived(rsend.at[0:nx - 1], rs)

    @pl.when(relay)
    def _():
        arrived(psend, ps)
        arrived(usend, us)
        arrived(lsend.at[0:nd - 1 - hz], ls)

    @pl.when(jnp.logical_not(relay))
    def _():
        arrived(rsend.at[nx - 1], ro)
        arrived(lsend.at[0:nd - 1], ls)


def fused(nx, ny, features, link_weight, link_row, link_col, link_live, bias):
    nd = nx * ny
    layers = bias.shape[0]
    block = link_weight.shape[-1]
    width = bias.shape[1] // block
    rows = features.shape[0]
    hz = ny // 2
    chunks = 2 * hz
    per = nd // chunks
    size = per * rows
    near = nx * hz
    steps = (layers - 1) * chunks
    bf16, f32 = jnp.bfloat16, jnp.float32
    vmem = pltpu.VMEM
    counts = pltpu.SMEM((layers, 1, nd), jnp.int32)
    dma = pltpu.SemaphoreType.DMA
    return pl.pallas_call(
        functools.partial(kernel, nx, ny),
        out_shape=vmem(features.shape, bf16),
        in_specs=[pl.BlockSpec(memory_space=pl.ANY)] * 6,
        out_specs=pl.BlockSpec(memory_space=vmem),
        scratch_shapes=[
            vmem(features.shape, bf16), counts, counts, counts, vmem(bias.shape, f32), dma((5,)),
            vmem((layers, nd, block, block), bf16), dma,
            vmem((nd, rows, width * block), bf16), dma, dma((chunks,)),
            vmem((width, rows * nd, block), bf16),
            vmem((8, block), f32), vmem((width, block), f32), vmem((nd, block), f32), dma, dma,
            vmem((hz, 8, block), f32), dma, dma, vmem((nd, width, block), f32), dma, dma,
            vmem((nd * nd, block), f32), vmem(((layers - 1) * hz * nd, 8, block), f32),
            vmem((near, steps, size, block), bf16), vmem((steps, near, size, block), bf16), dma, dma((steps,)),
            vmem((nx, steps, hz, size, block), bf16), vmem((steps, near, hz, size, block), bf16), dma, dma, dma((steps,)),
            vmem((steps, hz, width, size, block), bf16), vmem((steps, width, size, block), bf16), dma, dma((steps,)),
            vmem((nd, nd, rows, block), bf16), vmem((near, nd, rows, block), bf16), dma, dma,
            vmem((hz, GROUPS, near, nd // GROUPS, rows, block), bf16), dma((hz, GROUPS)),
            vmem((hz, nd, width, rows, block), bf16), vmem((nd, width, rows, block), bf16), dma, dma((GROUPS,)),
            vmem((nd * width, rows, block), f32),
        ],
        compiler_params=pltpu.CompilerParams(
            collective_id=0, has_side_effects=True, vmem_limit_bytes=60 * 1024 * 1024
        ),
    )(features, link_weight, link_row, jnp.transpose(link_col, (0, 2, 1)), link_live, bias)


def solution(mesh):
    placed = (
        P(("nx", "ny", "img"), None),
        P(None, ("nx", "ny"), None, None, None),
        P(None, ("nx", "ny"), None),
        P(None, None, ("nx", "ny")),
        P(None, ("nx", "ny"), None),
        P(None, ("nx", "ny")),
    )
    nx, ny = mesh.shape["nx"], mesh.shape["ny"]

    def run(features, link_weight, link_row, link_col, link_live, bias):
        block = link_weight.shape[-1]
        rows = features.shape[0]
        width = bias.shape[1] // block
        fits = (
            rows % 8 == 0 and nx % 2 == 0 and ny % 2 == 0 and block == 128
            and nx * ny <= 32 and nx * ny % GROUPS == 0 and bias.shape[0] <= 8 and (nx * rows) % 16 == 0 and bias.shape[0] > 1
        )
        step = functools.partial(fused, nx, ny) if fits else local
        return step(features, link_weight, link_row, link_col, link_live, bias)

    return jax.shard_map(
        run, mesh=mesh, in_specs=placed, out_specs=P(("nx", "ny", "img"), None), check_vma=False
    )
```
